128 devices in a mesh: dp: 2 (over core), ep: 64 (over x, y, z).
Axes of the slice: x: 4, y: 4, z: 4, core: 2. Of those that a mesh axis runs over, the one named last changes fastest.
Arguments:
- x: bfloat16 [2, 64, 256, 2048], P('dp', 'ep'), parts along dimension 0
- expert: int32 [2, 64, 256, 6], P('dp', 'ep'), parts along dimension 0
- slot: int32 [2, 64, 256, 6], P('dp', 'ep'), parts along dimension 0
- gate: float32 [2, 64, 256, 6], P('dp', 'ep'), parts along dimension 0
- w_gate: bfloat16 [64, 2048, 1408], P('ep')
- w_up: bfloat16 [64, 2048, 1408], P('ep')
- w_down: bfloat16 [64, 1408, 2048], P('ep')
- s_gate: bfloat16 [2048, 2816], replicated
- s_up: bfloat16 [2048, 2816], replicated
- s_down: bfloat16 [2816, 2048], replicated
Outputs:
- y: bfloat16 [2, 64, 256, 2048], P('dp', 'ep'), parts along dimension 0
There are 2 independent parts. The reference program is written for one: setup_inputs(seed, part) draws one part's arguments, and reference() takes and returns one part's arrays. A program takes and returns all parts, laid end to end along the dimension named above; an argument that names none is the same for every part.
All inputs are finite; a program needn't handle non-finite values.
Results may differ from the reference program's by a relative error of at most 0.009.
Values are sent between devices in bfloat16 or wider.
A program may use at most 1.5 GiB of HBM per device.

```python
import jax
import jax.numpy as jnp

MEMBERS = 64
TOKENS = 256
D = 2048
FF = 1408
TOP = 6
EXPERTS = 64
SHARED_FF = 2816
SLOTS = 5 * TOKENS * TOP // (4 * EXPERTS)


def setup_inputs(seed: int = 0, part: int = 0) -> dict:
    own, k1, k2, k3, k4, k5, k6 = jax.random.split(jax.random.key(seed), 7)
    kx, ke, kl, kg = jax.random.split(jax.random.fold_in(own, part), 4)
    devices = (1, MEMBERS)
    place = jax.random.permutation(kl, jnp.arange(EXPERTS, dtype=jnp.uint32))
    slow = ((EXPERTS + (9 * place) % EXPERTS) << ((9 * place) // EXPERTS)) // EXPERTS
    wait = (jax.random.bits(ke, (*devices, TOKENS, EXPERTS), jnp.uint32) >> 10) * slow
    expert = jnp.argsort(wait, axis=-1)[..., :TOP].astype(jnp.int32)
    chosen = jax.nn.one_hot(expert, EXPERTS, dtype=jnp.int32)
    in_line = jnp.cumsum(chosen.reshape(*devices, TOKENS * TOP, EXPERTS), axis=2) - 1
    slot = jnp.sum(in_line.reshape(chosen.shape) * chosen, axis=-1)

    def one(key, rows, columns):
        return (jax.random.normal(key, (rows, columns), jnp.float32) * rows**-0.5).astype(jnp.bfloat16)

    def weights(key, rows, columns):
        return jax.lax.map(lambda k: one(k, rows, columns), jax.random.split(key, EXPERTS))

    return {
        "x": jax.random.normal(kx, (*devices, TOKENS, D), jnp.float32).astype(jnp.bfloat16),
        "expert": expert,
        "slot": slot,
        "gate": jax.nn.softmax(jax.random.normal(kg, expert.shape, jnp.float32)),
        "w_gate": weights(k1, D, FF),
        "w_up": weights(k2, D, FF),
        "w_down": weights(k3, FF, D),
        "s_gate": one(k4, D, SHARED_FF),
        "s_up": one(k5, D, SHARED_FF),
        "s_down": one(k6, SHARED_FF, D),
    }


def einsum(form, a, b):
    return jnp.einsum(form, a.astype(jnp.float32), b.astype(jnp.float32))


def for_all(x, s_gate, s_up, s_down):
    h = jax.nn.silu(einsum("...d,df->...f", x, s_gate)) * einsum("...d,df->...f", x, s_up)
    return einsum("...f,fd->...d", h.astype(jnp.bfloat16), s_down)


def reference(x, expert, slot, gate, w_gate, w_up, w_down, s_gate, s_up, s_down):
    to_expert = jax.nn.one_hot(expert, EXPERTS, dtype=jnp.bfloat16)
    to_slot = jax.nn.one_hot(slot, SLOTS, dtype=jnp.bfloat16)
    weighted = to_expert * gate[..., None].astype(jnp.bfloat16)
    dispatch = einsum("abtke,abtkc->abtec", to_expert, to_slot).astype(jnp.bfloat16)
    combine = einsum("abtke,abtkc->abtec", weighted, to_slot).astype(jnp.bfloat16)
    z = einsum("abtec,abtd->aebcd", dispatch, x).astype(jnp.bfloat16)
    h = jax.nn.silu(einsum("aebcd,edf->aebcf", z, w_gate))
    h = (h * einsum("aebcd,edf->aebcf", z, w_up)).astype(jnp.bfloat16)
    out = einsum("aebcf,efd->aebcd", h, w_down).astype(jnp.bfloat16)
    y = einsum("abtec,aebcd->abtd", combine, out)
    return (y + for_all(x, s_gate, s_up, s_down)).astype(jnp.bfloat16)
```

```python
import functools

import jax
import jax.numpy as jnp
from jax import lax
from jax.experimental import pallas as pl
from jax.experimental.pallas import tpu as pltpu
from jax.sharding import PartitionSpec as P

MESH = pl.DeviceIdType.MESH
BF16, F32 = jnp.bfloat16, jnp.float32
S = 16
HALVES = 2
SPAN = S * HALVES
ALL = slice(None)


def silu_mul(g, u):
    return (jax.nn.silu(g) * u).astype(BF16)


def kernel(R, parts, shared_tile, top, names, *refs):
    (x_ref, m_ref, wg_hbm, wu_hbm, wd_hbm, sg_hbm, su_hbm, sd_hbm, y_ref) = refs[:9]
    xa, g_buf, h_buf, z_buf, ps = refs[9:12], refs[12:15], refs[15:18], refs[18:21], refs[21:24]
    (meta, wg, wu, wd, zcat, hb, yacc, sgb, sub, sdb,
     w_sem, sh_sem, m_s, m_r, a_s, a_r, b_s, b_r, c_s, c_r, c2_s, c2_r, b2_s, b2_r, a2_s, a2_r, h_free, g_free) = refs[24:]
    dp_axis, ep_axis = names
    T = x_ref.shape[0]
    FF = wg.shape[1]
    KR = R * R * S
    dp, me = lax.axis_index(dp_axis), lax.axis_index(ep_axis)
    pos = (me // (R * R), lax.rem(me // R, R), lax.rem(me, R))
    unit = (R * R, R, 1)
    edges = [0]
    for c in parts:
        edges.append(edges[-1] + c)
    cols = [slice(edges[k], edges[k + 1]) for k in range(3)]

    def peer(axis, r):
        return me + (lax.rem(pos[axis] + r, R) - pos[axis]) * unit[axis]

    def zsl(k, a, b, c):
        i = [None] * 3
        i[k], i[(k + 1) % 3], i[(k + 2) % 3] = a, b, c
        return tuple(i)

    def hsl(k, a, b):
        return (a, b) if k < 2 else (b, a)

    def send(src, dst, s, r, axis, step):
        pltpu.make_async_remote_copy(
            src_ref=src, dst_ref=dst, send_sem=s, recv_sem=r,
            device_id=(dp, peer(axis, step)), device_id_type=MESH,
        ).start()

    def pend(ref, s, r):
        return pltpu.make_async_remote_copy(
            src_ref=ref, dst_ref=ref, send_sem=s, recv_sem=r,
            device_id=(dp, peer(0, 1)), device_id_type=MESH,
        )

    def whole(k, h):
        return g_buf[k].at[h, 1:R]

    n_sh = sg_hbm.shape[1] // shared_tile

    def sh_copies(j, slot):
        at = pl.ds(pl.multiple_of(j * shared_tile, shared_tile), shared_tile)
        return (
            pltpu.make_async_copy(sg_hbm.at[:, at], sgb.at[slot], sh_sem.at[slot, 0]),
            pltpu.make_async_copy(su_hbm.at[:, at], sub.at[slot], sh_sem.at[slot, 1]),
            pltpu.make_async_copy(sd_hbm.at[at], sdb.at[slot], sh_sem.at[slot, 2]),
        )

    for c in sh_copies(0, 0):
        c.start()

    barrier = pltpu.get_barrier_semaphore()
    for axis in range(3):
        for r in range(1, R):
            pl.semaphore_signal(barrier, inc=1, device_id=(dp, peer(axis, r)), device_id_type=MESH)
    pl.semaphore_wait(barrier, 3 * (R - 1))

    for k in range(3):
        for r in range(1, R):
            send(m_ref, meta.at[k, R - r], m_s.at[k], m_r.at[k], k, r)
    for r in range(1, R):
        for k in range(3):
            send(x_ref.at[:, cols[k]], xa[k].at[R - r], a_s.at[k], a_r.at[k], k, r)
    for k in range(3):
        meta[k, 0] = m_ref[...]
        xa[k][0] = x_ref[:, cols[k]]

    yacc[...] = jnp.zeros_like(yacc)

    @pl.loop(0, n_sh)
    def _(j):
        slot = lax.rem(j, 2)
        for c in sh_copies(j, slot):
            c.wait()

        @pl.when(j + 1 < n_sh)
        def _():
            for c in sh_copies(j + 1, 1 - slot):
                c.start()

        g = jnp.dot(x_ref[...], sgb[slot], preferred_element_type=F32)
        u = jnp.dot(x_ref[...], sub[slot], preferred_element_type=F32)
        yacc[...] += jnp.dot(silu_mul(g, u), sdb[slot], preferred_element_type=F32)

    w_copies = [
        pltpu.make_async_copy(src, dst, w_sem.at[i])
        for i, (src, dst) in enumerate(((wg_hbm, wg), (wu_hbm, wu), (wd_hbm, wd)))
    ]
    for c in w_copies:
        c.start()

    def slot_ids(k, h):
        row = lax.broadcasted_iota(jnp.int32, (KR, T), 0)
        rb, rc, s = row // (R * S), lax.rem(row // S, R), lax.rem(row, S)
        b, c = (k + 1) % 3, (k + 2) % 3
        e = pos[k] * unit[k] + lax.rem(rb + pos[b], R) * unit[b] + lax.rem(rc + pos[c], R) * unit[c]
        return (e * SPAN + s + h * S).astype(F32)

    def gather(k, h):
        ids = slot_ids(k, h)

        @pl.loop(0, R)
        def _(ra):
            hit = ids == meta[k, ra, 0:1, :]
            for j in range(1, top):
                hit = hit | (ids == meta[k, ra, j:j + 1, :])
            pick = jnp.where(hit, 1.0, 0.0).astype(BF16)
            rows = jnp.dot(pick, xa[k][ra], preferred_element_type=F32).astype(BF16)
            rows = rows.reshape(R, R, S, parts[k])
            g_buf[k][h, 1:R, :, ra] = rows[1:]
            z_buf[k][(h,) + zsl(k, ra, 0, 0)] = rows[0, 0]
            h_buf[k][(h, ALL) + hsl(k, ra, 0)] = rows[0, 1:]

    def send_b(k, h):
        for rb in range(1, R):
            to = R - rb
            send(g_buf[k].at[h, rb, 1:R], h_buf[k].at[(h, ALL) + hsl(k, ALL, to)],
                 b_s.at[k, h], b_r.at[k, h], (k + 1) % 3, rb)
            send(g_buf[k].at[h, rb, 0], z_buf[k].at[(h,) + zsl(k, ALL, to, 0)],
                 b_s.at[k, h], b_r.at[k, h], (k + 1) % 3, rb)

    def relay_c(h):
        for k in range(3):
            pend(whole(k, h), b_s.at[k, h], b_r.at[k, h]).wait_recv()
            for rc in range(1, R):
                send(h_buf[k].at[h, rc - 1], z_buf[k].at[(h,) + zsl(k, ALL, ALL, R - rc)],
                     c_s.at[k, h], c_r.at[k, h], (k + 2) % 3, rc)

    for k in range(3):
        pend(meta.at[k, 1:R], m_s.at[k], m_r.at[k]).wait_recv()
        pend(xa[k].at[1:R], a_s.at[k], a_r.at[k]).wait_recv()
        gather(k, 0)
        send_b(k, 0)
    for k in range(3):
        gather(k, 1)
    relay_c(0)
    for k in range(3):
        send_b(k, 1)

    for c in w_copies:
        c.wait()

    def send_c2(h, rx):
        for k in range(3):
            s, r, axis = c2_s.at[k, h], c2_r.at[k, h], (k + 2) % 3
            z, hh, g = z_buf[k], h_buf[k], g_buf[k]
            if k == 0:
                for rc in range(1, R):
                    send(z.at[h, rx, 1:R, rc], hh.at[h, R - rc - 1, rx, 1:R], s, r, axis, rc)
                    send(z.at[h, rx, 0, rc], g.at[h, 0, R - rc, rx], s, r, axis, rc)
            elif k == 1:
                @pl.when(rx > 0)
                def _():
                    send(z.at[h, rx, :, 1:R], hh.at[h, R - rx - 1, :, 1:R], s, r, axis, rx)
                    send(z.at[h, rx, :, 0], g.at[h, 0, R - rx], s, r, axis, rx)
            else:
                @pl.when(rx > 0)
                def _():
                    for rc in range(1, R):
                        send(z.at[h, rx, rc], hh.at[h, R - rc - 1, rx], s, r, axis, rc)

                @pl.when(rx == 0)
                def _():
                    for rc in range(1, R):
                        send(z.at[h, rx, rc], g.at[h, 0, R - rc], s, r, axis, rc)

    def relay_b2(h):
        for k in range(3):
            pend(whole(k, h), c2_s.at[k, h], c2_r.at[k, h]).wait_recv()
            pl.semaphore_wait(g_free.at[k, h], R - 1)
            for rb in range(1, R):
                s, r, axis, to = b2_s.at[k, h], b2_r.at[k, h], (k + 1) % 3, R - rb
                send(h_buf[k].at[(h, ALL) + hsl(k, ALL, rb)], g_buf[k].at[h, to, 1:R], s, r, axis, rb)
                send(z_buf[k].at[(h,) + zsl(k, ALL, rb, 0)], g_buf[k].at[h, to, 0], s, r, axis, rb)

    wide = [(n, min(512, FF - n)) for n in range(0, FF, 512)]

    @pl.loop(0, HALVES * R)
    def _(t):
        h, rx = t // R, lax.rem(t, R)

        @pl.when(rx == 0)
        def _():
            for k in range(3):
                pend(whole(k, h), c_s.at[k, h], c_r.at[k, h]).wait_recv()
            for k in range(3):
                pend(whole(k, h), c_s.at[k, h], c_r.at[k, h]).wait_send()
                pend(whole(k, h), b_s.at[k, h], b_r.at[k, h]).wait_send()
                for free, axis in ((h_free, k + 2), (g_free, k + 1)):
                    for r in range(1, R):
                        pl.semaphore_signal(free.at[k, h], inc=1, device_id=(dp, peer(axis % 3, r)), device_id_type=MESH)

        for k in range(3):
            zcat[:, cols[k]] = z_buf[k][h, rx].reshape(KR, parts[k])
        for n, w in wide:
            g = jnp.dot(zcat[...], wg[:, n:n + w], preferred_element_type=F32)
            u = jnp.dot(zcat[...], wu[:, n:n + w], preferred_element_type=F32)
            hb[:, n:n + w] = silu_mul(g, u)
        for k in range(3):
            o = jnp.dot(hb[...], wd[:, cols[k]], preferred_element_type=F32)
            z_buf[k][h, rx] = o.astype(BF16).reshape(R, R, S, parts[k])

        @pl.when(rx == 0)
        def _():
            for k in range(3):
                pl.semaphore_wait(h_free.at[k, h], R - 1)

        send_c2(h, rx)

        @pl.when(t == R // 2 - 1)
        def _():
            relay_c(1)

        @pl.when(t == R + R // 2 - 1)
        def _():
            relay_b2(0)

    def own_rows(k, h):
        g_buf[k][h, 0, 0] = z_buf[k][(h,) + zsl(k, ALL, 0, 0)]

    def weighted(k, ra, h):
        ids = slot_ids(k, h)
        w = jnp.zeros((KR, T), F32)
        for j in range(top):
            w += jnp.where(ids == meta[k, ra, j:j + 1, :], meta[k, ra, 8 + j:9 + j, :], 0.0)
        rows = g_buf[k][h, :, :, ra].reshape(KR, parts[k])
        return lax.dot_general(w.astype(BF16), rows, (((0,), (0,)), ((), ())), preferred_element_type=F32)

    for k in range(3):
        for h in range(HALVES):
            own_rows(k, h)
    for k in range(3):
        pend(whole(k, 0), b2_s.at[k, 0], b2_r.at[k, 0]).wait_recv()
        yacc[:, cols[k]] += weighted(k, 0, 0)
    relay_b2(1)
    for k in range(3):
        pend(whole(k, 1), b2_s.at[k, 1], b2_r.at[k, 1]).wait_recv()

        @pl.loop(1, R)
        def _(ra):
            ps[k][ra - 1] = (weighted(k, ra, 0) + weighted(k, ra, 1)).astype(BF16)
            send(ps[k].at[ra - 1], xa[k].at[R - ra], a2_s.at[k], a2_r.at[k], k, ra)

    for k in range(3):
        yacc[:, cols[k]] += weighted(k, 0, 1)
    for k in range(3):
        pend(xa[k].at[1:R], a2_s.at[k], a2_r.at[k]).wait_recv()
        total = yacc[:, cols[k]]
        for ra in range(1, R):
            total += xa[k][ra].astype(F32)
        y_ref[:, cols[k]] = total.astype(BF16)

    for k in range(3):
        pend(meta.at[k, 1:R], m_s.at[k], m_r.at[k]).wait_send()
        pend(xa[k].at[1:R], a_s.at[k], a_r.at[k]).wait_send()
        pend(xa[k].at[1:R], a2_s.at[k], a2_r.at[k]).wait_send()
        for h in range(HALVES):
            for s, r in ((c2_s, c2_r), (b2_s, b2_r)):
                pend(whole(k, h), s.at[k, h], r.at[k, h]).wait_send()


def split(d):
    tiles = d // 128
    low = tiles // 3
    sizes = [low, low, low]
    for i in range(tiles - 3 * low):
        sizes[2 - i] += 1
    return [128 * n for n in sizes]


def solution(mesh):
    names = ("dp", "ep")

    def step(x, expert, slot, gate, w_gate, w_up, w_down, s_gate, s_up, s_down):
        R = round(mesh.shape["ep"] ** (1 / 3))
        T, D = x.shape[2:]
        top, members = expert.shape[-1], mesh.shape["ep"]
        FF, SFF = w_gate.shape[-1], s_gate.shape[-1]
        slots = 5 * T * top // (4 * members)
        parts = split(D)
        x, expert, slot, gate = x[0, 0], expert[0, 0], slot[0, 0], gate[0, 0]
        key = jnp.where(slot < slots, expert * SPAN + slot, -1).astype(F32)
        weight = gate.astype(BF16).astype(F32)
        m = jnp.concatenate([jnp.pad(key.T, ((0, 8 - top), (0, 0))), jnp.pad(weight.T, ((0, 8 - top), (0, 0)))], 0)
        any_space = pl.BlockSpec(memory_space=pl.ANY)
        vmem = pl.BlockSpec(memory_space=pltpu.VMEM)
        tile = min(256, SFF)
        dma = pltpu.SemaphoreType.DMA
        scratch = (
            [pltpu.VMEM((R, T, c), BF16) for c in parts]
            + [pltpu.VMEM((HALVES, R, R, R, S, c), BF16) for c in parts]
            + [pltpu.VMEM((HALVES, R - 1, R, R, S, c), BF16) for c in parts]
            + [pltpu.VMEM((HALVES, R, R, R, S, c), BF16) for c in parts]
            + [pltpu.VMEM((R - 1, T, c), BF16) for c in parts]
            + [pltpu.VMEM((3, R, 16, T), F32)]
            + [pltpu.VMEM((D, FF), BF16), pltpu.VMEM((D, FF), BF16), pltpu.VMEM((FF, D), BF16)]
            + [pltpu.VMEM((R * R * S, D), BF16), pltpu.VMEM((R * R * S, FF), BF16), pltpu.VMEM((T, D), F32)]
            + [pltpu.VMEM((2, D, tile), BF16), pltpu.VMEM((2, D, tile), BF16), pltpu.VMEM((2, tile, D), BF16)]
            + [dma((3,)), dma((2, 3))]
            + [dma((3,))] * 4 + [dma((3, HALVES))] * 8 + [dma((3,))] * 2
            + [pltpu.SemaphoreType.REGULAR((3, HALVES))] * 2
        )
        y = pl.pallas_call(
            functools.partial(kernel, R, parts, tile, top, names),
            out_shape=jax.ShapeDtypeStruct((T, D), BF16),
            in_specs=[vmem, vmem] + [any_space] * 6,
            out_specs=vmem,
            scratch_shapes=scratch,
            compiler_params=pltpu.CompilerParams(
                collective_id=0, has_side_effects=True, vmem_limit_bytes=67043328
            ),
            name="moe",
        )(x, m, w_gate[0], w_up[0], w_down[0], s_gate, s_up, s_down)
        return y[None, None]

    tok = P("dp", "ep", None, None)
    exp = P("ep", None, None)
    rep = P(None, None)
    return jax.shard_map(
        step, mesh=mesh,
        in_specs=(tok, tok, tok, tok, exp, exp, exp, rep, rep, rep),
        out_specs=tok, check_vma=False,
    )
```

```python
import functools

import jax
import jax.numpy as jnp
from jax import lax
from jax.experimental import pallas as pl
from jax.experimental.pallas import tpu as pltpu
from jax.sharding import PartitionSpec as P

MESH = pl.DeviceIdType.MESH
BF16, F32 = jnp.bfloat16, jnp.float32
S = 16
HALVES = 2
SPAN = S * HALVES
ALL = slice(None)


def silu_mul(g, u):
    return (jax.nn.silu(g) * u).astype(BF16)


def kernel(R, parts, shared_tile, top, names, *refs):
    (x_ref, m_ref, wg_hbm, wu_hbm, wd_hbm, sg_hbm, su_hbm, sd_hbm, y_ref) = refs[:9]
    xa, g_buf, h_buf, z_buf, ps = refs[9:12], refs[12:15], refs[15:18], refs[18:21], refs[21:24]
    (meta, wg, wu, wd, zcat, hb, yacc, sgb, sub, sdb,
     w_sem, sh_sem, m_s, m_r, a_s, a_r, b_s, b_r, c_s, c_r, c2_s, c2_r, b2_s, b2_r, a2_s, a2_r, h_free, g_free) = refs[24:]
    dp_axis, ep_axis = names
    T = x_ref.shape[0]
    FF = wg.shape[1]
    KR = R * R * S
    dp, me = lax.axis_index(dp_axis), lax.axis_index(ep_axis)
    pos = (me // (R * R), lax.rem(me // R, R), lax.rem(me, R))
    unit = (R * R, R, 1)
    edges = [0]
    for c in parts:
        edges.append(edges[-1] + c)
    cols = [slice(edges[k], edges[k + 1]) for k in range(3)]

    order = sorted(range(3), key=lambda k: -parts[k])
    near = sorted(range(1, R), key=lambda r: (min(r, R - r), -r))

    def peer(axis, r):
        return me + (lax.rem(pos[axis] + r, R) - pos[axis]) * unit[axis]

    def zsl(k, a, b, c):
        i = [None] * 3
        i[k], i[(k + 1) % 3], i[(k + 2) % 3] = a, b, c
        return tuple(i)

    def hsl(k, a, b):
        return (a, b) if k < 2 else (b, a)

    def send(src, dst, s, r, axis, step):
        pltpu.make_async_remote_copy(
            src_ref=src, dst_ref=dst, send_sem=s, recv_sem=r,
            device_id=(dp, peer(axis, step)), device_id_type=MESH,
        ).start()

    def pend(ref, s, r):
        return pltpu.make_async_remote_copy(
            src_ref=ref, dst_ref=ref, send_sem=s, recv_sem=r,
            device_id=(dp, peer(0, 1)), device_id_type=MESH,
        )

    def whole(k, h):
        return g_buf[k].at[h, 1:R]

    n_sh = sg_hbm.shape[1] // shared_tile

    def sh_copies(j, slot):
        at = pl.ds(pl.multiple_of(j * shared_tile, shared_tile), shared_tile)
        return (
            pltpu.make_async_copy(sg_hbm.at[:, at], sgb.at[slot], sh_sem.at[slot, 0]),
            pltpu.make_async_copy(su_hbm.at[:, at], sub.at[slot], sh_sem.at[slot, 1]),
            pltpu.make_async_copy(sd_hbm.at[at], sdb.at[slot], sh_sem.at[slot, 2]),
        )

    for c in sh_copies(0, 0):
        c.start()

    def shared(j):
        slot = lax.rem(j, 2)
        for c in sh_copies(j, slot):
            c.wait()

        @pl.when(j + 1 < n_sh)
        def _():
            for c in sh_copies(j + 1, 1 - slot):
                c.start()

        g = jnp.dot(x_ref[...], sgb[slot], preferred_element_type=F32)
        u = jnp.dot(x_ref[...], sub[slot], preferred_element_type=F32)
        yacc[...] += jnp.dot(silu_mul(g, u), sdb[slot], preferred_element_type=F32)

    def slot_ids(k, h):
        row = lax.broadcasted_iota(jnp.int32, (KR, T), 0)
        rb, rc, s = row // (R * S), lax.rem(row // S, R), lax.rem(row, S)
        b, c = (k + 1) % 3, (k + 2) % 3
        e = pos[k] * unit[k] + lax.rem(rb + pos[b], R) * unit[b] + lax.rem(rc + pos[c], R) * unit[c]
        return (e * SPAN + s + h * S).astype(F32)

    def gather(k, h, ra, ids):
        hit = ids == meta[k, ra, 0:1, :]
        for j in range(1, top):
            hit = hit | (ids == meta[k, ra, j:j + 1, :])
        pick = jnp.where(hit, 1.0, 0.0).astype(BF16)
        rows = jnp.dot(pick, xa[k][ra], preferred_element_type=F32).astype(BF16)
        rows = rows.reshape(R, R, S, parts[k])
        g_buf[k][h, 1:R, :, ra] = rows[1:]
        z_buf[k][(h,) + zsl(k, ra, 0, 0)] = rows[0, 0]
        h_buf[k][(h, ALL) + hsl(k, ra, 0)] = rows[0, 1:]

    def send_b(k, h, ra):
        for rb in near:
            to = R - rb
            send(g_buf[k].at[h, rb, 1:R, ra], h_buf[k].at[(h, ALL) + hsl(k, ra, to)],
                 b_s.at[k, h], b_r.at[k, h, ra], (k + 1) % 3, rb)
            send(g_buf[k].at[h, rb, 0, ra], z_buf[k].at[(h,) + zsl(k, ra, to, 0)],
                 b_s.at[k, h], b_r.at[k, h, ra], (k + 1) % 3, rb)

    @jax.named_scope("relay_c")
    def relay_c(h, ra):
        for k in order:
            pend(g_buf[k].at[h, 1:R, :, 0], b_s.at[k, h], b_r.at[k, h, ra]).wait_recv()
            for rc in near:
                send(h_buf[k].at[(h, rc - 1) + hsl(k, ra, ALL)], z_buf[k].at[(h,) + zsl(k, ra, ALL, R - rc)],
                     c_s.at[k, h], c_r.at[k, h], (k + 2) % 3, rc)

    barrier = pltpu.get_barrier_semaphore()
    for axis in range(3):
        for r in range(1, R):
            pl.semaphore_signal(barrier, inc=1, device_id=(dp, peer(axis, r)), device_id_type=MESH)

    for k in range(3):
        meta[k, 0] = m_ref[...]
        xa[k][0] = x_ref[:, cols[k]]
    yacc[...] = jnp.zeros_like(yacc)

    @pl.loop(0, HALVES)
    @jax.named_scope("gather")
    def _(h):
        for k in order:
            gather(k, h, 0, slot_ids(k, h))

    with jax.named_scope("barrier"):
        pl.semaphore_wait(barrier, 3 * (R - 1))

    for k in order:
        for r in near:
            send(m_ref, meta.at[k, R - r], m_s.at[k], m_r.at[k], k, r)
    for r in near:
        for k in order:
            send(x_ref.at[:, cols[k]], xa[k].at[R - r], a_s.at[k], a_r.at[k], k, r)
    for k in order:
        send_b(k, 0, 0)

    pl.loop(0, n_sh - R)(jax.named_scope("shared")(shared))

    w_copies = [
        pltpu.make_async_copy(src, dst, w_sem.at[i])
        for i, (src, dst) in enumerate(((wg_hbm, wg), (wu_hbm, wu), (wd_hbm, wd)))
    ]
    for c in w_copies:
        c.start()

    for k in order:
        with jax.named_scope("wait_a"):
            pend(meta.at[k, 1:R], m_s.at[k], m_r.at[k]).wait_recv()
            pend(xa[k].at[1:R], a_s.at[k], a_r.at[k]).wait_recv()
        ids = slot_ids(k, 0)

        @pl.loop(1, R)
        @jax.named_scope("gather")
        def _(ra):
            gather(k, 0, ra, ids)
            send_b(k, 0, ra)

    for k in order:
        ids = slot_ids(k, 1)

        @pl.loop(1, R)
        @jax.named_scope("gather")
        def _(ra):
            gather(k, 1, ra, ids)

    @pl.loop(0, R)
    def _(ra):
        with jax.named_scope("shared"):
            shared(n_sh - R + ra)
        relay_c(0, ra)
        for k in order:
            send_b(k, 1, ra)

    for c in w_copies:
        c.wait()

    def send_c2(h, rx):
        for k in order:
            s, axis = c2_s.at[k, h], (k + 2) % 3
            z, hh, g = z_buf[k], h_buf[k], g_buf[k]
            if k == 0:
                for rc in near:
                    send(z.at[h, rx, 1:R, rc], hh.at[h, R - rc - 1, rx, 1:R], s, c2_r.at[k, h, R - rc], axis, rc)
                    send(z.at[h, rx, 0, rc], g.at[h, 0, R - rc, rx], s, c2_r.at[k, h, R - rc], axis, rc)
            elif k == 1:
                @pl.when(rx > 0)
                def _():
                    send(z.at[h, rx, :, 1:R], hh.at[h, R - rx - 1, :, 1:R], s, c2_r.at[k, h, R - rx], axis, rx)
                    send(z.at[h, rx, :, 0], g.at[h, 0, R - rx], s, c2_r.at[k, h, R - rx], axis, rx)
            else:
                @pl.when(rx > 0)
                def _():
                    for rc in near:
                        send(z.at[h, rx, rc], hh.at[h, R - rc - 1, rx], s, c2_r.at[k, h, R - rc], axis, rc)

                @pl.when(rx == 0)
                def _():
                    for rc in near:
                        send(z.at[h, rx, rc], g.at[h, 0, R - rc], s, c2_r.at[k, h, R - rc], axis, rc)

    def own_b2(h):
        for k in order:
            pl.semaphore_wait(g_free.at[k, h], R - 1)
            for rb in near:
                send(z_buf[k].at[(h,) + zsl(k, ALL, rb, 0)], g_buf[k].at[h, R - rb, 0],
                     b2_s.at[k, h], b2_r.at[k, h], (k + 1) % 3, rb)

    @jax.named_scope("relay_b2")
    def relay_b2(h):
        for ce in range(R - 1, 0, -1):
            for k in order:
                pend(g_buf[k].at[h, 1], c2_s.at[k, h], c2_r.at[k, h, ce]).wait_recv()
                for rb in near:
                    send(h_buf[k].at[(h, ce - 1) + hsl(k, ALL, rb)], g_buf[k].at[h, R - rb, ce],
                         b2_s.at[k, h], b2_r.at[k, h], (k + 1) % 3, rb)

    wide = [(n, min(512, FF - n)) for n in range(0, FF, 512)]

    @pl.loop(0, HALVES * R)
    def _(t):
        h, rx = t // R, lax.rem(t, R)

        @pl.when(rx == 0)
        @jax.named_scope("wait_c")
        def _():
            for k in range(3):
                pend(whole(k, h), c_s.at[k, h], c_r.at[k, h]).wait_recv()
            for k in range(3):
                pend(whole(k, h), c_s.at[k, h], c_r.at[k, h]).wait_send()
                pend(whole(k, h), b_s.at[k, h], b_r.at[k, h]).wait_send()
                for free, axis in ((h_free, k + 2), (g_free, k + 1)):
                    for r in range(1, R):
                        pl.semaphore_signal(free.at[k, h], inc=1, device_id=(dp, peer(axis % 3, r)), device_id_type=MESH)

        @pl.when(t == 0)
        def _():
            @pl.loop(0, R // 2)
            def _(ra):
                relay_c(1, ra)

        with jax.named_scope("up"):
            for k in range(3):
                zcat[:, cols[k]] = z_buf[k][h, rx].reshape(KR, parts[k])
            for n, w in wide:
                g = jnp.dot(zcat[...], wg[:, n:n + w], preferred_element_type=F32)
                u = jnp.dot(zcat[...], wu[:, n:n + w], preferred_element_type=F32)
                hb[:, n:n + w] = silu_mul(g, u)
        with jax.named_scope("down"):
            for k in range(3):
                o = jnp.dot(hb[...], wd[:, cols[k]], preferred_element_type=F32)
                z_buf[k][h, rx] = o.astype(BF16).reshape(R, R, S, parts[k])

        @pl.when(rx == 0)
        def _():
            for k in range(3):
                pl.semaphore_wait(h_free.at[k, h], R - 1)

        send_c2(h, rx)

        @pl.when(t == 0)
        def _():
            @pl.loop(R // 2, R)
            def _(ra):
                relay_c(1, ra)

        @pl.when(rx == R - 1)
        def _():
            own_b2(h)

        @pl.when(t == R + R // 2 - 1)
        def _():
            relay_b2(0)

    def own_rows(k, h):
        g_buf[k][h, 0, 0] = z_buf[k][(h,) + zsl(k, ALL, 0, 0)]

    def weighted(k, ra, h):
        ids = slot_ids(k, h)
        w = jnp.zeros((KR, T), F32)
        for j in range(top):
            w += jnp.where(ids == meta[k, ra, j:j + 1, :], meta[k, ra, 8 + j:9 + j, :], 0.0)
        rows = g_buf[k][h, :, :, ra].reshape(KR, parts[k])
        return lax.dot_general(w.astype(BF16), rows, (((0,), (0,)), ((), ())), preferred_element_type=F32)

    relay_b2(1)
    for k in order:
        for h in range(HALVES):
            own_rows(k, h)
    for k in order:
        with jax.named_scope("wait_b2"):
            pend(whole(k, 0), b2_s.at[k, 0], b2_r.at[k, 0]).wait_recv()
        with jax.named_scope("weigh_own"):
            yacc[:, cols[k]] += weighted(k, 0, 0)
    for k in order:
        with jax.named_scope("wait_b2"):
            pend(whole(k, 1), b2_s.at[k, 1], b2_r.at[k, 1]).wait_recv()

        @pl.loop(1, R)
        @jax.named_scope("weigh")
        def _(ra):
            ps[k][ra - 1] = (weighted(k, ra, 0) + weighted(k, ra, 1)).astype(BF16)
            send(ps[k].at[ra - 1], xa[k].at[R - ra], a2_s.at[k], a2_r.at[k], k, ra)

    for k in order:
        with jax.named_scope("weigh_own"):
            yacc[:, cols[k]] += weighted(k, 0, 1)
    for k in order:
        with jax.named_scope("wait_a2"):
            pend(xa[k].at[1:R], a2_s.at[k], a2_r.at[k]).wait_recv()
        total = yacc[:, cols[k]]
        for ra in range(1, R):
            total += xa[k][ra].astype(F32)
        y_ref[:, cols[k]] = total.astype(BF16)

    for k in range(3):
        pend(meta.at[k, 1:R], m_s.at[k], m_r.at[k]).wait_send()
        pend(xa[k].at[1:R], a_s.at[k], a_r.at[k]).wait_send()
        pend(xa[k].at[1:R], a2_s.at[k], a2_r.at[k]).wait_send()
        for h in range(HALVES):
            for s, r in ((c2_s, c2_r), (b2_s, b2_r)):
                pend(whole(k, h), s.at[k, h], r.at[k, h]).wait_send()


def split(d):
    tiles = d // 128
    low = tiles // 3
    sizes = [low, low, low]
    for i in range(tiles - 3 * low):
        sizes[2 - i] += 1
    return [128 * n for n in sizes]


def solution(mesh):
    names = ("dp", "ep")

    def step(x, expert, slot, gate, w_gate, w_up, w_down, s_gate, s_up, s_down):
        R = round(mesh.shape["ep"] ** (1 / 3))
        T, D = x.shape[2:]
        top, members = expert.shape[-1], mesh.shape["ep"]
        FF, SFF = w_gate.shape[-1], s_gate.shape[-1]
        slots = 5 * T * top // (4 * members)
        parts = split(D)
        x, expert, slot, gate = x[0, 0], expert[0, 0], slot[0, 0], gate[0, 0]
        key = jnp.where(slot < slots, expert * SPAN + slot, -1).astype(F32)
        weight = gate.astype(BF16).astype(F32)
        m = jnp.concatenate([jnp.pad(key.T, ((0, 8 - top), (0, 0))), jnp.pad(weight.T, ((0, 8 - top), (0, 0)))], 0)
        any_space = pl.BlockSpec(memory_space=pl.ANY)
        vmem = pl.BlockSpec(memory_space=pltpu.VMEM)
        tile = min(256, SFF)
        dma = pltpu.SemaphoreType.DMA
        scratch = (
            [pltpu.VMEM((R, T, c), BF16) for c in parts]
            + [pltpu.VMEM((HALVES, R, R, R, S, c), BF16) for c in parts]
            + [pltpu.VMEM((HALVES, R - 1, R, R, S, c), BF16) for c in parts]
            + [pltpu.VMEM((HALVES, R, R, R, S, c), BF16) for c in parts]
            + [pltpu.VMEM((R - 1, T, c), BF16) for c in parts]
            + [pltpu.VMEM((3, R, 16, T), F32)]
            + [pltpu.VMEM((D, FF), BF16), pltpu.VMEM((D, FF), BF16), pltpu.VMEM((FF, D), BF16)]
            + [pltpu.VMEM((R * R * S, D), BF16), pltpu.VMEM((R * R * S, FF), BF16), pltpu.VMEM((T, D), F32)]
            + [pltpu.VMEM((2, D, tile), BF16), pltpu.VMEM((2, D, tile), BF16), pltpu.VMEM((2, tile, D), BF16)]
            + [dma((3,)), dma((2, 3))]
            + [dma((3,))] * 4
            + [dma((3, HALVES)), dma((3, HALVES, R)), dma((3, HALVES)), dma((3, HALVES))]
            + [dma((3, HALVES)), dma((3, HALVES, R)), dma((3, HALVES)), dma((3, HALVES))] + [dma((3,))] * 2
            + [pltpu.SemaphoreType.REGULAR((3, HALVES))] * 2
        )
        y = pl.pallas_call(
            functools.partial(kernel, R, parts, tile, top, names),
            out_shape=jax.ShapeDtypeStruct((T, D), BF16),
            in_specs=[vmem, vmem] + [any_space] * 6,
            out_specs=vmem,
            scratch_shapes=scratch,
            compiler_params=pltpu.CompilerParams(
                collective_id=0, has_side_effects=True, vmem_limit_bytes=67043328
            ),
            name="moe",
        )(x, m, w_gate[0], w_up[0], w_down[0], s_gate, s_up, s_down)
        return y[None, None]

    tok = P("dp", "ep", None, None)
    exp = P("ep", None, None)
    rep = P(None, None)
    return jax.shard_map(
        step, mesh=mesh,
        in_specs=(tok, tok, tok, tok, exp, exp, exp, rep, rep, rep),
        out_specs=tok, check_vma=False,
    )
```

```python
import functools

import jax
import jax.numpy as jnp
from jax import lax
from jax.experimental import pallas as pl
from jax.experimental.pallas import tpu as pltpu
from jax.sharding import PartitionSpec as P

MESH = pl.DeviceIdType.MESH
BF16, F32 = jnp.bfloat16, jnp.float32
S = 16
HALVES = 2
SPAN = S * HALVES
ALL = slice(None)


def silu_mul(g, u):
    return (jax.nn.silu(g) * u).astype(BF16)


def kernel(R, parts, shared_tile, top, names, *refs):
    (x_ref, m_ref, wg_hbm, wu_hbm, wd_hbm, sg_hbm, su_hbm, sd_hbm, y_ref) = refs[:9]
    xa, g_buf, h_buf, z_buf, ps = refs[9:12], refs[12:15], refs[15:18], refs[18:21], refs[21:24]
    (meta, wg, wu, wd, zcat, hb, yacc, sgb, sub, sdb,
     w_sem, sh_sem, m_s, m_r, a_s, a_r, b_s, b_r, c_s, c_r, c2_s, c2_r, b2_s, b2_r, a2_s, a2_r, ah_r, h_free, g_free) = refs[24:]
    dp_axis, ep_axis = names
    T = x_ref.shape[0]
    FF = wg.shape[1]
    KR = R * R * S
    dp, me = lax.axis_index(dp_axis), lax.axis_index(ep_axis)
    pos = (me // (R * R), lax.rem(me // R, R), lax.rem(me, R))
    unit = (R * R, R, 1)
    edges = [0]
    for c in parts:
        edges.append(edges[-1] + c)
    cols = [slice(edges[k], edges[k + 1]) for k in range(3)]

    order = sorted(range(3), key=lambda k: -parts[k])
    near = sorted(range(1, R), key=lambda r: (min(r, R - r), -r))
    ring4 = R == 4
    lo, hi = pl.ds(0, T // 2), pl.ds(T // 2, T // 2)

    def peer(axis, r):
        return me + (lax.rem(pos[axis] + r, R) - pos[axis]) * unit[axis]

    def zsl(k, a, b, c):
        i = [None] * 3
        i[k], i[(k + 1) % 3], i[(k + 2) % 3] = a, b, c
        return tuple(i)

    def hsl(k, a, b):
        return (a, b) if k < 2 else (b, a)

    def send(src, dst, s, r, axis, step):
        pltpu.make_async_remote_copy(
            src_ref=src, dst_ref=dst, send_sem=s, recv_sem=r,
            device_id=(dp, peer(axis, step)), device_id_type=MESH,
        ).start()

    def pend(ref, s, r):
        return pltpu.make_async_remote_copy(
            src_ref=ref, dst_ref=ref, send_sem=s, recv_sem=r,
            device_id=(dp, peer(0, 1)), device_id_type=MESH,
        )

    def whole(k, h):
        return g_buf[k].at[h, 1:R]

    n_sh = sg_hbm.shape[1] // shared_tile

    def sh_copies(j, slot):
        at = pl.ds(pl.multiple_of(j * shared_tile, shared_tile), shared_tile)
        return (
            pltpu.make_async_copy(sg_hbm.at[:, at], sgb.at[slot], sh_sem.at[slot, 0]),
            pltpu.make_async_copy(su_hbm.at[:, at], sub.at[slot], sh_sem.at[slot, 1]),
            pltpu.make_async_copy(sd_hbm.at[at], sdb.at[slot], sh_sem.at[slot, 2]),
        )

    for c in sh_copies(0, 0):
        c.start()

    def shared(j):
        slot = lax.rem(j, 2)
        for c in sh_copies(j, slot):
            c.wait()

        @pl.when(j + 1 < n_sh)
        def _():
            for c in sh_copies(j + 1, 1 - slot):
                c.start()

        g = jnp.dot(x_ref[...], sgb[slot], preferred_element_type=F32)
        u = jnp.dot(x_ref[...], sub[slot], preferred_element_type=F32)
        yacc[...] += jnp.dot(silu_mul(g, u), sdb[slot], preferred_element_type=F32)

    def slot_ids(k, h):
        row = lax.broadcasted_iota(jnp.int32, (KR, T), 0)
        rb, rc, s = row // (R * S), lax.rem(row // S, R), lax.rem(row, S)
        b, c = (k + 1) % 3, (k + 2) % 3
        e = pos[k] * unit[k] + lax.rem(rb + pos[b], R) * unit[b] + lax.rem(rc + pos[c], R) * unit[c]
        return (e * SPAN + s + h * S).astype(F32)

    def gather(k, h, ra, ids):
        hit = ids == meta[k, ra, 0:1, :]
        for j in range(1, top):
            hit = hit | (ids == meta[k, ra, j:j + 1, :])
        pick = jnp.where(hit, 1.0, 0.0).astype(BF16)
        rows = jnp.dot(pick, xa[k][ra], preferred_element_type=F32).astype(BF16)
        rows = rows.reshape(R, R, S, parts[k])
        g_buf[k][h, 1:R, :, ra] = rows[1:]
        z_buf[k][(h,) + zsl(k, ra, 0, 0)] = rows[0, 0]
        h_buf[k][(h, ALL) + hsl(k, ra, 0)] = rows[0, 1:]

    def send_b(k, h, ra):
        for rb in near:
            to = R - rb
            send(g_buf[k].at[h, rb, 1:R, ra], h_buf[k].at[(h, ALL) + hsl(k, ra, to)],
                 b_s.at[k, h], b_r.at[k, h, ra], (k + 1) % 3, rb)
            send(g_buf[k].at[h, rb, 0, ra], z_buf[k].at[(h,) + zsl(k, ra, to, 0)],
                 b_s.at[k, h], b_r.at[k, h, ra], (k + 1) % 3, rb)

    @jax.named_scope("relay_c")
    def relay_c(h, ra):
        for k in order:
            pend(g_buf[k].at[h, 1:R, :, 0], b_s.at[k, h], b_r.at[k, h, ra]).wait_recv()
            for rc in near:
                send(h_buf[k].at[(h, rc - 1) + hsl(k, ra, ALL)], z_buf[k].at[(h,) + zsl(k, ra, ALL, R - rc)],
                     c_s.at[k, h], c_r.at[k, h], (k + 2) % 3, rc)

    barrier = pltpu.get_barrier_semaphore()
    for axis in range(3):
        for r in range(1, R):
            pl.semaphore_signal(barrier, inc=1, device_id=(dp, peer(axis, r)), device_id_type=MESH)

    for k in range(3):
        meta[k, 0] = m_ref[...]
        xa[k][0] = x_ref[:, cols[k]]
    yacc[...] = jnp.zeros_like(yacc)

    @pl.loop(0, HALVES)
    @jax.named_scope("gather")
    def _(h):
        for k in order:
            gather(k, h, 0, slot_ids(k, h))

    with jax.named_scope("barrier"):
        pl.semaphore_wait(barrier, 3 * (R - 1))

    for k in order:
        for r in near:
            send(m_ref, meta.at[k, R - r], m_s.at[k], m_r.at[k], k, r)
    for r in near:
        if not ring4 or r != 2:
            for k in order:
                send(x_ref.at[:, cols[k]], xa[k].at[R - r], a_s.at[k], a_r.at[k, R - r], k, r)
    for k in order:
        send_b(k, 0, 0)

    early = max(n_sh - R - 2, 0)
    pl.loop(0, early)(jax.named_scope("shared")(shared))

    @jax.named_scope("wait_a")
    def wait_a(k, ra):
        pend(xa[k].at[ra], a_s.at[k], a_r.at[k, ra]).wait_recv()

    @jax.named_scope("gather")
    def gather_all(h, ra, go):
        for k in order:
            gather(k, h, ra, slot_ids(k, h))
            if go:
                send_b(k, h, ra)

    for k in order:
        with jax.named_scope("wait_m"):
            pend(meta.at[k, 1:R], m_s.at[k], m_r.at[k]).wait_recv()
    if ring4:
        for k in order:
            wait_a(k, 3)
            send(xa[k].at[3, lo], xa[k].at[2, lo], a_s.at[k], a_r.at[k, 2], k, 1)
            wait_a(k, 1)
            send(xa[k].at[1, hi], xa[k].at[2, hi], a_s.at[k], a_r.at[k, 2], k, 3)
        seq = [0, 3, 1, 2]

        @pl.loop(0, 2)
        def _(i):
            gather_all(0, 3 - 2 * i, True)
    else:
        seq = list(range(R))
    pl.loop(early, n_sh - R)(jax.named_scope("shared")(shared))

    w_copies = [
        pltpu.make_async_copy(src, dst, w_sem.at[i])
        for i, (src, dst) in enumerate(((wg_hbm, wg), (wu_hbm, wu), (wd_hbm, wd)))
    ]
    for c in w_copies:
        c.start()

    for ra in [2] if ring4 else seq[1:]:
        for k in order:
            wait_a(k, ra)
        gather_all(0, ra, True)

    @pl.loop(1, R)
    def _(ra):
        gather_all(1, ra, False)

    @pl.loop(0, R)
    def _(i):
        with jax.named_scope("shared"):
            shared(n_sh - R + i)
        for step, ra in enumerate(seq):
            @pl.when(i == step)
            def _():
                relay_c(0, ra)
                for k in order:
                    send_b(k, 1, ra)

    for c in w_copies:
        c.wait()

    def send_c2(h, rx):
        for k in order:
            s, axis = c2_s.at[k, h], (k + 2) % 3
            z, hh, g = z_buf[k], h_buf[k], g_buf[k]
            if k == 0:
                for rc in near:
                    send(z.at[h, rx, 1:R, rc], hh.at[h, R - rc - 1, rx, 1:R], s, c2_r.at[k, h, R - rc], axis, rc)
                    send(z.at[h, rx, 0, rc], g.at[h, 0, R - rc, rx], s, c2_r.at[k, h, R - rc], axis, rc)
            elif k == 1:
                @pl.when(rx > 0)
                def _():
                    send(z.at[h, rx, :, 1:R], hh.at[h, R - rx - 1, :, 1:R], s, c2_r.at[k, h, R - rx], axis, rx)
                    send(z.at[h, rx, :, 0], g.at[h, 0, R - rx], s, c2_r.at[k, h, R - rx], axis, rx)
            else:
                @pl.when(rx > 0)
                def _():
                    for rc in near:
                        send(z.at[h, rx, rc], hh.at[h, R - rc - 1, rx], s, c2_r.at[k, h, R - rc], axis, rc)

                @pl.when(rx == 0)
                def _():
                    for rc in near:
                        send(z.at[h, rx, rc], g.at[h, 0, R - rc], s, c2_r.at[k, h, R - rc], axis, rc)

    def own_b2(h):
        for k in order:
            pl.semaphore_wait(g_free.at[k, h], R - 1)
            for rb in near:
                send(z_buf[k].at[(h,) + zsl(k, ALL, rb, 0)], g_buf[k].at[h, R - rb, 0],
                     b2_s.at[k, h], b2_r.at[k, h], (k + 1) % 3, rb)

    @jax.named_scope("relay_b2")
    def relay_b2(h):
        for ce in range(R - 1, 0, -1):
            for k in order:
                pend(g_buf[k].at[h, 1], c2_s.at[k, h], c2_r.at[k, h, ce]).wait_recv()
                for rb in near:
                    send(h_buf[k].at[(h, ce - 1) + hsl(k, ALL, rb)], g_buf[k].at[h, R - rb, ce],
                         b2_s.at[k, h], b2_r.at[k, h], (k + 1) % 3, rb)

    wide = [(n, min(512, FF - n)) for n in range(0, FF, 512)]

    @pl.loop(0, HALVES * R)
    def _(t):
        h, rx = t // R, lax.rem(t, R)

        @pl.when(rx == 0)
        @jax.named_scope("wait_c")
        def _():
            for k in range(3):
                pend(whole(k, h), c_s.at[k, h], c_r.at[k, h]).wait_recv()
            @pl.when(t == 0)
            def _():
                for k in range(3):
                    pend(xa[k].at[1:R], a_s.at[k], a2_r.at[k]).wait_send()

            for k in range(3):
                pend(whole(k, h), c_s.at[k, h], c_r.at[k, h]).wait_send()
                pend(whole(k, h), b_s.at[k, h], b_r.at[k, h]).wait_send()
                for free, axis in ((h_free, k + 2), (g_free, k + 1)):
                    for r in range(1, R):
                        pl.semaphore_signal(free.at[k, h], inc=1, device_id=(dp, peer(axis % 3, r)), device_id_type=MESH)

        @pl.when(t == 0)
        def _():
            for ra in seq[:R // 2]:
                relay_c(1, ra)

        with jax.named_scope("up"):
            for k in range(3):
                zcat[:, cols[k]] = z_buf[k][h, rx].reshape(KR, parts[k])
            for n, w in wide:
                g = jnp.dot(zcat[...], wg[:, n:n + w], preferred_element_type=F32)
                u = jnp.dot(zcat[...], wu[:, n:n + w], preferred_element_type=F32)
                hb[:, n:n + w] = silu_mul(g, u)
        with jax.named_scope("down"):
            for k in range(3):
                o = jnp.dot(hb[...], wd[:, cols[k]], preferred_element_type=F32)
                z_buf[k][h, rx] = o.astype(BF16).reshape(R, R, S, parts[k])

        @pl.when(rx == 0)
        def _():
            for k in range(3):
                pl.semaphore_wait(h_free.at[k, h], R - 1)

        send_c2(h, rx)

        @pl.when(t == 0)
        def _():
            for ra in seq[R // 2:]:
                relay_c(1, ra)

        @pl.when(rx == R - 1)
        def _():
            own_b2(h)

        @pl.when(t == R + R // 2 - 1)
        def _():
            relay_b2(0)

    def own_rows(k, h):
        g_buf[k][h, 0, 0] = z_buf[k][(h,) + zsl(k, ALL, 0, 0)]

    def weighted(k, ra, h, at=pl.ds(0, T)):
        ids = slot_ids(k, h)[:, :at.size]
        w = jnp.zeros((KR, at.size), F32)
        for j in range(top):
            gate = meta[k, ra, 8 + j:9 + j, at].astype(BF16).astype(F32)
            w += jnp.where(ids == meta[k, ra, j:j + 1, at], gate, 0.0)
        rows = g_buf[k][h, :, :, ra].reshape(KR, parts[k])
        return lax.dot_general(w.astype(BF16), rows, (((0,), (0,)), ((), ())), preferred_element_type=F32)

    def partial(k, ra, at=pl.ds(0, T)):
        return weighted(k, ra, 0, at) + weighted(k, ra, 1, at)

    relay_b2(1)
    for k in order:
        for h in range(HALVES):
            own_rows(k, h)
    for k in order:
        with jax.named_scope("wait_b2"):
            pend(whole(k, 0), b2_s.at[k, 0], b2_r.at[k, 0]).wait_recv()
        with jax.named_scope("weigh_own"):
            yacc[:, cols[k]] += weighted(k, 0, 0)
    for k in order:
        with jax.named_scope("wait_b2"):
            pend(whole(k, 1), b2_s.at[k, 1], b2_r.at[k, 1]).wait_recv()

    def send_a2(k, ra, at):
        send(ps[k].at[ra - 1, at], xa[k].at[R - ra, at], a2_s.at[k], a2_r.at[k], k, ra)

    if ring4:
        for k in order:
            with jax.named_scope("weigh_far"):
                ps[k][1] = partial(k, 2).astype(BF16)
            send(ps[k].at[1, lo], xa[k].at[2, lo], a2_s.at[k], ah_r.at[k, 0], k, 1)
            send(ps[k].at[1, hi], xa[k].at[2, hi], a2_s.at[k], ah_r.at[k, 1], k, 3)
        for k in order:
            with jax.named_scope("weigh_near"):
                ps[k][0, hi] = partial(k, 1, hi).astype(BF16)
                send_a2(k, 1, hi)
                ps[k][2, lo] = partial(k, 3, lo).astype(BF16)
                send_a2(k, 3, lo)
        for k in order:
            for i, (ra, at) in enumerate(((1, lo), (3, hi))):
                with jax.named_scope("weigh_sum"):
                    own = partial(k, ra, at)
                    pend(xa[k].at[2, at], a2_s.at[k], ah_r.at[k, i]).wait_recv()
                    ps[k][ra - 1, at] = (own + xa[k][2, at].astype(F32)).astype(BF16)
                    send_a2(k, ra, at)
    else:
        for k in order:
            for ra in range(1, R):
                ps[k][ra - 1] = partial(k, ra).astype(BF16)
                send_a2(k, ra, pl.ds(0, T))
    senders = (1, 3) if ring4 else tuple(range(1, R))

    for k in order:
        with jax.named_scope("weigh_own"):
            yacc[:, cols[k]] += weighted(k, 0, 1)
    for k in order:
        with jax.named_scope("wait_a2"):
            pend(xa[k].at[0:len(senders)], a2_s.at[k], a2_r.at[k]).wait_recv()
        total = yacc[:, cols[k]]
        for ra in senders:
            total += xa[k][ra].astype(F32)
        y_ref[:, cols[k]] = total.astype(BF16)

    for k in range(3):
        pend(meta.at[k, 1:R], m_s.at[k], m_r.at[k]).wait_send()
        pend(xa[k].at[1:R], a2_s.at[k], a2_r.at[k]).wait_send()
        for h in range(HALVES):
            for s, r in ((c2_s, c2_r), (b2_s, b2_r)):
                pend(whole(k, h), s.at[k, h], r.at[k, h]).wait_send()


def split(d):
    tiles = d // 128
    low = tiles // 3
    sizes = [low, low, low]
    for i in range(tiles - 3 * low):
        sizes[2 - i] += 1
    return [128 * n for n in sizes]


def solution(mesh):
    names = ("dp", "ep")

    def step(x, expert, slot, gate, w_gate, w_up, w_down, s_gate, s_up, s_down):
        R = round(mesh.shape["ep"] ** (1 / 3))
        T, D = x.shape[2:]
        top, members = expert.shape[-1], mesh.shape["ep"]
        FF, SFF = w_gate.shape[-1], s_gate.shape[-1]
        slots = 5 * T * top // (4 * members)
        parts = split(D)
        x, expert, slot, gate = x[0, 0], expert[0, 0], slot[0, 0], gate[0, 0]
        key = jnp.where(slot < slots, expert * SPAN + slot, -1).astype(F32)
        m = jnp.pad(key.T, ((0, 16 - top), (0, 0))) + jnp.pad(gate.T, ((8, 8 - top), (0, 0)))
        any_space = pl.BlockSpec(memory_space=pl.ANY)
        vmem = pl.BlockSpec(memory_space=pltpu.VMEM)
        tile = min(256, SFF)
        dma = pltpu.SemaphoreType.DMA
        scratch = (
            [pltpu.VMEM((R, T, c), BF16) for c in parts]
            + [pltpu.VMEM((HALVES, R, R, R, S, c), BF16) for c in parts]
            + [pltpu.VMEM((HALVES, R - 1, R, R, S, c), BF16) for c in parts]
            + [pltpu.VMEM((HALVES, R, R, R, S, c), BF16) for c in parts]
            + [pltpu.VMEM((R - 1, T, c), BF16) for c in parts]
            + [pltpu.VMEM((3, R, 16, T), F32)]
            + [pltpu.VMEM((D, FF), BF16), pltpu.VMEM((D, FF), BF16), pltpu.VMEM((FF, D), BF16)]
            + [pltpu.VMEM((R * R * S, D), BF16), pltpu.VMEM((R * R * S, FF), BF16), pltpu.VMEM((T, D), F32)]
            + [pltpu.VMEM((2, D, tile), BF16), pltpu.VMEM((2, D, tile), BF16), pltpu.VMEM((2, tile, D), BF16)]
            + [dma((3,)), dma((2, 3))]
            + [dma((3,))] * 3 + [dma((3, R))]
            + [dma((3, HALVES)), dma((3, HALVES, R)), dma((3, HALVES)), dma((3, HALVES))]
            + [dma((3, HALVES)), dma((3, HALVES, R)), dma((3, HALVES)), dma((3, HALVES))] + [dma((3,))] * 2 + [dma((3, 2))]
            + [pltpu.SemaphoreType.REGULAR((3, HALVES))] * 2
        )
        y = pl.pallas_call(
            functools.partial(kernel, R, parts, tile, top, names),
            out_shape=jax.ShapeDtypeStruct((T, D), BF16),
            in_specs=[vmem, vmem] + [any_space] * 6,
            out_specs=vmem,
            scratch_shapes=scratch,
            compiler_params=pltpu.CompilerParams(
                collective_id=0, has_side_effects=True, vmem_limit_bytes=67043328
            ),
            name="moe",
        )(x, m, w_gate[0], w_up[0], w_down[0], s_gate, s_up, s_down)
        return y[None, None]

    tok = P("dp", "ep", None, None)
    exp = P("ep", None, None)
    rep = P(None, None)
    return jax.shard_map(
        step, mesh=mesh,
        in_specs=(tok, tok, tok, tok, exp, exp, exp, rep, rep, rep),
        out_specs=tok, check_vma=False,
    )
```

```python
import functools

import jax
import jax.numpy as jnp
from jax import lax
from jax.experimental import pallas as pl
from jax.experimental.pallas import tpu as pltpu
from jax.sharding import PartitionSpec as P

MESH = pl.DeviceIdType.MESH
BF16, F32 = jnp.bfloat16, jnp.float32
S = 16
HALVES = 2
SPAN = S * HALVES
ALL = slice(None)


def silu_mul(g, u):
    return (jax.nn.silu(g) * u).astype(BF16)


def kernel(R, parts, shared_tile, top, slots, names, *refs):
    (x_ref, e_ref, s_ref, gate_ref, wg_hbm, wu_hbm, wd_hbm, sg_hbm, su_hbm, sd_hbm, y_ref) = refs[:11]
    xa, g_buf, h_buf, z_buf, ps, own = (refs[i:i + 3] for i in range(11, 29, 3))
    (m_ref, meta, wg, wu, wd, zcat, hb, yacc, sgb, sub, sdb,
     w_sem, sh_sem, m_s, m_r, a_s, a_r, b_s, b_r, c_s, c_r, c2_s, c2_r, b2_s, b2_r, a2_s, a2_r, ah_r, h_free, g_free) = refs[29:]
    dp_axis, ep_axis = names
    T = x_ref.shape[0]
    FF = wg.shape[1]
    KR = R * R * S
    dp, me = lax.axis_index(dp_axis), lax.axis_index(ep_axis)
    pos = (me // (R * R), lax.rem(me // R, R), lax.rem(me, R))
    unit = (R * R, R, 1)
    edges = [0]
    for c in parts:
        edges.append(edges[-1] + c)
    cols = [slice(edges[k], edges[k + 1]) for k in range(3)]

    order = sorted(range(3), key=lambda k: -parts[k])
    near = sorted(range(1, R), key=lambda r: (min(r, R - r), -r))
    ring4 = R == 4
    lo, hi = pl.ds(0, T // 2), pl.ds(T // 2, T // 2)

    def peer(axis, r):
        return me + (lax.rem(pos[axis] + r, R) - pos[axis]) * unit[axis]

    def zsl(k, a, b, c):
        i = [None] * 3
        i[k], i[(k + 1) % 3], i[(k + 2) % 3] = a, b, c
        return tuple(i)

    def hsl(k, a, b):
        return (a, b) if k < 2 else (b, a)

    def send(src, dst, s, r, axis, step):
        pltpu.make_async_remote_copy(
            src_ref=src, dst_ref=dst, send_sem=s, recv_sem=r,
            device_id=(dp, peer(axis, step)), device_id_type=MESH,
        ).start()

    def pend(ref, s, r):
        return pltpu.make_async_remote_copy(
            src_ref=ref, dst_ref=ref, send_sem=s, recv_sem=r,
            device_id=(dp, peer(0, 1)), device_id_type=MESH,
        )

    def whole(k, h):
        return g_buf[k].at[h, 1:R]

    n_sh = sg_hbm.shape[1] // shared_tile

    def sh_copies(j, slot):
        at = pl.ds(pl.multiple_of(j * shared_tile, shared_tile), shared_tile)
        return (
            pltpu.make_async_copy(sg_hbm.at[:, at], sgb.at[slot], sh_sem.at[slot, 0]),
            pltpu.make_async_copy(su_hbm.at[:, at], sub.at[slot], sh_sem.at[slot, 1]),
            pltpu.make_async_copy(sd_hbm.at[at], sdb.at[slot], sh_sem.at[slot, 2]),
        )

    for c in sh_copies(0, 0):
        c.start()

    def shared(j):
        slot = lax.rem(j, 2)
        for c in sh_copies(j, slot):
            c.wait()

        @pl.when(j + 1 < n_sh)
        def _():
            for c in sh_copies(j + 1, 1 - slot):
                c.start()

        g = jnp.dot(x_ref[...], sgb[slot], preferred_element_type=F32)
        u = jnp.dot(x_ref[...], sub[slot], preferred_element_type=F32)
        yacc[...] += jnp.dot(silu_mul(g, u), sdb[slot], preferred_element_type=F32)

    def slot_ids(k, h):
        row = lax.broadcasted_iota(jnp.int32, (KR, T), 0)
        rb, rc, s = row // (R * S), lax.rem(row // S, R), lax.rem(row, S)
        b, c = (k + 1) % 3, (k + 2) % 3
        e = pos[k] * unit[k] + lax.rem(rb + pos[b], R) * unit[b] + lax.rem(rc + pos[c], R) * unit[c]
        return (e * SPAN + s + h * S).astype(F32)

    def gather(k, h, ra, ids):
        hit = ids == meta[k, ra, 0:1, :]
        for j in range(1, top):
            hit = hit | (ids == meta[k, ra, j:j + 1, :])
        pick = jnp.where(hit, 1.0, 0.0).astype(BF16)
        rows = jnp.dot(pick, xa[k][ra], preferred_element_type=F32).astype(BF16)
        rows = rows.reshape(R, R, S, parts[k])
        g_buf[k][h, 1:R, :, ra] = rows[1:]
        z_buf[k][(h,) + zsl(k, ra, 0, 0)] = rows[0, 0]
        h_buf[k][(h, ALL) + hsl(k, ra, 0)] = rows[0, 1:]

    def send_b(k, h, ra):
        for rb in near:
            to = R - rb
            send(g_buf[k].at[h, rb, 1:R, ra], h_buf[k].at[(h, ALL) + hsl(k, ra, to)],
                 b_s.at[k, h], b_r.at[k, h, ra], (k + 1) % 3, rb)
            send(g_buf[k].at[h, rb, 0, ra], z_buf[k].at[(h,) + zsl(k, ra, to, 0)],
                 b_s.at[k, h], b_r.at[k, h, ra], (k + 1) % 3, rb)

    @jax.named_scope("relay_c")
    def relay_c(h, ra):
        for k in order:
            pend(g_buf[k].at[h, 1:R, :, 0], b_s.at[k, h], b_r.at[k, h, ra]).wait_recv()
            for rc in near:
                send(h_buf[k].at[(h, rc - 1) + hsl(k, ra, ALL)], z_buf[k].at[(h,) + zsl(k, ra, ALL, R - rc)],
                     c_s.at[k, h], c_r.at[k, h], (k + 2) % 3, rc)

    barrier = pltpu.get_barrier_semaphore()
    for axis in range(3):
        for r in range(1, R):
            pl.semaphore_signal(barrier, inc=1, device_id=(dp, peer(axis, r)), device_id_type=MESH)

    m_ref[...] = jnp.zeros_like(m_ref)
    for j in range(top):
        m_ref[j:j + 1, :] = jnp.where(s_ref[j] < slots, e_ref[j] * SPAN + s_ref[j], -1).astype(F32)
        m_ref[8 + j:9 + j, :] = gate_ref[j].astype(BF16).astype(F32)
    for k in range(3):
        meta[k, 0] = m_ref[...]
        xa[k][0] = x_ref[:, cols[k]]
    yacc[...] = jnp.zeros_like(yacc)

    @pl.loop(0, HALVES)
    @jax.named_scope("gather")
    def _(h):
        for k in order:
            gather(k, h, 0, slot_ids(k, h))

    with jax.named_scope("barrier"):
        pl.semaphore_wait(barrier, 3 * (R - 1))

    for k in order:
        for r in near:
            send(m_ref, meta.at[k, R - r], m_s.at[k], m_r.at[k], k, r)
    for r in near:
        if not ring4 or r != 2:
            for k in order:
                send(x_ref.at[:, cols[k]], xa[k].at[R - r], a_s.at[k], a_r.at[k, R - r], k, r)
    for k in order:
        send_b(k, 0, 0)

    early = max(n_sh - R - 2, 0)
    pl.loop(0, early)(jax.named_scope("shared")(shared))

    @jax.named_scope("wait_a")
    def wait_a(k, ra):
        pend(xa[k].at[ra], a_s.at[k], a_r.at[k, ra]).wait_recv()

    @jax.named_scope("gather")
    def gather_all(h, ra, go):
        for k in order:
            gather(k, h, ra, slot_ids(k, h))
            if go:
                send_b(k, h, ra)

    for k in order:
        with jax.named_scope("wait_m"):
            pend(meta.at[k, 1:R], m_s.at[k], m_r.at[k]).wait_recv()
    if ring4:
        for k in order:
            wait_a(k, 3)
            send(xa[k].at[3, lo], xa[k].at[2, lo], a_s.at[k], a_r.at[k, 2], k, 1)
            wait_a(k, 1)
            send(xa[k].at[1, hi], xa[k].at[2, hi], a_s.at[k], a_r.at[k, 2], k, 3)
        seq = [0, 3, 1, 2]

        @pl.loop(0, 2)
        def _(i):
            gather_all(0, 3 - 2 * i, True)
    else:
        seq = list(range(R))
    pl.loop(early, n_sh - R)(jax.named_scope("shared")(shared))

    w_copies = [
        pltpu.make_async_copy(src, dst, w_sem.at[i])
        for i, (src, dst) in enumerate(((wg_hbm, wg), (wu_hbm, wu), (wd_hbm, wd)))
    ]
    for c in w_copies:
        c.start()

    for ra in [2] if ring4 else seq[1:]:
        for k in order:
            wait_a(k, ra)
        gather_all(0, ra, True)

    @pl.loop(1, R)
    def _(ra):
        gather_all(1, ra, False)

    @pl.loop(0, R)
    def _(i):
        with jax.named_scope("shared"):
            shared(n_sh - R + i)
        for step, ra in enumerate(seq):
            @pl.when(i == step)
            def _():
                relay_c(0, ra)
                for k in order:
                    send_b(k, 1, ra)

    for c in w_copies:
        c.wait()

    def send_c2(h, rx):
        for k in order:
            s, axis = c2_s.at[k, h], (k + 2) % 3
            z, hh, g = z_buf[k], h_buf[k], g_buf[k]
            if k == 0:
                for rc in near:
                    send(z.at[h, rx, 1:R, rc], hh.at[h, R - rc - 1, rx, 1:R], s, c2_r.at[k, h, R - rc], axis, rc)
                    send(z.at[h, rx, 0, rc], g.at[h, 0, R - rc, rx], s, c2_r.at[k, h, R - rc], axis, rc)
            elif k == 1:
                @pl.when(rx > 0)
                def _():
                    send(z.at[h, rx, :, 1:R], hh.at[h, R - rx - 1, :, 1:R], s, c2_r.at[k, h, R - rx], axis, rx)
                    send(z.at[h, rx, :, 0], g.at[h, 0, R - rx], s, c2_r.at[k, h, R - rx], axis, rx)
            else:
                @pl.when(rx > 0)
                def _():
                    for rc in near:
                        send(z.at[h, rx, rc], hh.at[h, R - rc - 1, rx], s, c2_r.at[k, h, R - rc], axis, rc)

                @pl.when(rx == 0)
                def _():
                    for rc in near:
                        send(z.at[h, rx, rc], g.at[h, 0, R - rc], s, c2_r.at[k, h, R - rc], axis, rc)

    def own_b2(h):
        for k in order:
            pl.semaphore_wait(g_free.at[k, h], R - 1)
            for rb in near:
                send(z_buf[k].at[(h,) + zsl(k, ALL, rb, 0)], g_buf[k].at[h, R - rb, 0],
                     b2_s.at[k, h], b2_r.at[k, h], (k + 1) % 3, rb)

    @jax.named_scope("relay_b2")
    def relay_b2(h):
        for ce in range(R - 1, 0, -1):
            for k in order:
                pend(g_buf[k].at[h, 1], c2_s.at[k, h], c2_r.at[k, h, ce]).wait_recv()
                for rb in near:
                    send(h_buf[k].at[(h, ce - 1) + hsl(k, ALL, rb)], g_buf[k].at[h, R - rb, ce],
                         b2_s.at[k, h], b2_r.at[k, h], (k + 1) % 3, rb)

    wide = [(n, min(512, FF - n)) for n in range(0, FF, 512)]

    @pl.loop(0, HALVES * R)
    def _(t):
        h, rx = t // R, lax.rem(t, R)

        @pl.when(rx == 0)
        @jax.named_scope("wait_c")
        def _():
            for k in range(3):
                pend(whole(k, h), c_s.at[k, h], c_r.at[k, h]).wait_recv()
            @pl.when(t == 0)
            def _():
                for k in range(3):
                    pend(xa[k].at[1:R], a_s.at[k], a2_r.at[k]).wait_send()

            for k in range(3):
                pend(whole(k, h), c_s.at[k, h], c_r.at[k, h]).wait_send()
                pend(whole(k, h), b_s.at[k, h], b_r.at[k, h]).wait_send()
                for free, axis in ((h_free, k + 2), (g_free, k + 1)):
                    for r in range(1, R):
                        pl.semaphore_signal(free.at[k, h], inc=1, device_id=(dp, peer(axis % 3, r)), device_id_type=MESH)

        @pl.when(t == 0)
        def _():
            for ra in seq[:R // 2]:
                relay_c(1, ra)

        with jax.named_scope("up"):
            for k in range(3):
                zcat[:, cols[k]] = z_buf[k][h, rx].reshape(KR, parts[k])
            for n, w in wide:
                g = jnp.dot(zcat[...], wg[:, n:n + w], preferred_element_type=F32)
                u = jnp.dot(zcat[...], wu[:, n:n + w], preferred_element_type=F32)
                hb[:, n:n + w] = silu_mul(g, u)
        with jax.named_scope("down"):
            for k in range(3):
                o = jnp.dot(hb[...], wd[:, cols[k]], preferred_element_type=F32)
                z_buf[k][h, rx] = o.astype(BF16).reshape(R, R, S, parts[k])

        @pl.when(rx == 0)
        def _():
            for k in range(3):
                pl.semaphore_wait(h_free.at[k, h], R - 1)

        send_c2(h, rx)

        @pl.when(t == 0)
        def _():
            for ra in seq[R // 2:]:
                relay_c(1, ra)

        @pl.when(rx == R - 1)
        def _():
            own_b2(h)

        @pl.when(t == R + R // 2 - 1)
        def _():
            relay_b2(0)

    def own_rows(k, h):
        g_buf[k][h, 0, 0] = z_buf[k][(h,) + zsl(k, ALL, 0, 0)]

    wide_w = HALVES * KR
    across = FF // wide_w

    def block(k, ra):
        i = k * R + ra
        return pl.ds(i // across * T, T), pl.ds(i % across * wide_w, wide_w)

    @jax.named_scope("weights")
    def build(k, ra):
        rows, columns = block(k, ra)
        for h in range(HALVES):
            ids = slot_ids(k, h)
            w = jnp.zeros((KR, T), F32)
            for j in range(top):
                w += jnp.where(ids == meta[k, ra, j:j + 1, :], meta[k, ra, 8 + j:9 + j, :], 0.0)
            wg[rows, pl.ds(columns.start + h * KR, KR)] = w.T.astype(BF16)

    def partial(k, ra):
        rows = g_buf[k][:, :, :, ra].reshape(wide_w, parts[k])
        return jnp.dot(wg[block(k, ra)], rows, preferred_element_type=F32)

    relay_b2(1)
    for k in order:
        for h in range(HALVES):
            own_rows(k, h)
    for ra in [2, 1, 3, 0] if ring4 else range(R):
        for k in order:
            build(k, ra)
    for k in order:
        with jax.named_scope("wait_b2"):
            pend(whole(k, 0), b2_s.at[k, 0], b2_r.at[k, 0]).wait_recv()
    for k in order:
        with jax.named_scope("wait_b2"):
            pend(whole(k, 1), b2_s.at[k, 1], b2_r.at[k, 1]).wait_recv()

    def send_a2(k, ra, at):
        send(ps[k].at[ra - 1, at], xa[k].at[R - ra, at], a2_s.at[k], a2_r.at[k], k, ra)

    if ring4:
        for k in order:
            with jax.named_scope("weigh_far"):
                ps[k][1] = partial(k, 2).astype(BF16)
            send(ps[k].at[1, lo], xa[k].at[2, lo], a2_s.at[k], ah_r.at[k, 0], k, 1)
            send(ps[k].at[1, hi], xa[k].at[2, hi], a2_s.at[k], ah_r.at[k, 1], k, 3)
        for k in order:
            with jax.named_scope("weigh_near"):
                for i, (ra, now, later) in enumerate(((1, slice(T // 2, T), slice(0, T // 2)), (3, slice(0, T // 2), slice(T // 2, T)))):
                    p = partial(k, ra)
                    ps[k][ra - 1, now] = p[now].astype(BF16)
                    send_a2(k, ra, hi if i == 0 else lo)
                    own[k][i] = p[later]
        for k in order:
            for i, (ra, at) in enumerate(((1, lo), (3, hi))):
                with jax.named_scope("weigh_sum"):
                    pend(xa[k].at[2, at], a2_s.at[k], ah_r.at[k, i]).wait_recv()
                    ps[k][ra - 1, at] = (own[k][i] + xa[k][2, at].astype(F32)).astype(BF16)
                    send_a2(k, ra, at)
    else:
        for k in order:
            for ra in range(1, R):
                ps[k][ra - 1] = partial(k, ra).astype(BF16)
                send_a2(k, ra, pl.ds(0, T))
    senders = (1, 3) if ring4 else tuple(range(1, R))

    for k in order:
        with jax.named_scope("weigh_own"):
            yacc[:, cols[k]] += partial(k, 0)
    for k in order:
        with jax.named_scope("wait_a2"):
            pend(xa[k].at[0:len(senders)], a2_s.at[k], a2_r.at[k]).wait_recv()
        total = yacc[:, cols[k]]
        for ra in senders:
            total += xa[k][ra].astype(F32)
        y_ref[:, cols[k]] = total.astype(BF16)

    for k in range(3):
        pend(meta.at[k, 1:R], m_s.at[k], m_r.at[k]).wait_send()
        pend(xa[k].at[1:R], a2_s.at[k], a2_r.at[k]).wait_send()
        for h in range(HALVES):
            for s, r in ((c2_s, c2_r), (b2_s, b2_r)):
                pend(whole(k, h), s.at[k, h], r.at[k, h]).wait_send()


def split(d):
    tiles = d // 128
    low = tiles // 3
    sizes = [low, low, low]
    for i in range(tiles - 3 * low):
        sizes[2 - i] += 1
    return [128 * n for n in sizes]


def solution(mesh):
    names = ("dp", "ep")

    def step(x, expert, slot, gate, w_gate, w_up, w_down, s_gate, s_up, s_down):
        R = round(mesh.shape["ep"] ** (1 / 3))
        T, D = x.shape[2:]
        top, members = expert.shape[-1], mesh.shape["ep"]
        FF, SFF = w_gate.shape[-1], s_gate.shape[-1]
        slots = 5 * T * top // (4 * members)
        parts = split(D)
        x, (expert, slot, gate) = x[0, 0], (v[0].transpose(2, 0, 1) for v in (expert, slot, gate))
        any_space = pl.BlockSpec(memory_space=pl.ANY)
        vmem = pl.BlockSpec(memory_space=pltpu.VMEM)
        tile = min(256, SFF)
        dma = pltpu.SemaphoreType.DMA
        scratch = (
            [pltpu.VMEM((R, T, c), BF16) for c in parts]
            + [pltpu.VMEM((HALVES, R, R, R, S, c), BF16) for c in parts]
            + [pltpu.VMEM((HALVES, R - 1, R, R, S, c), BF16) for c in parts]
            + [pltpu.VMEM((HALVES, R, R, R, S, c), BF16) for c in parts]
            + [pltpu.VMEM((R - 1, T, c), BF16) for c in parts]
            + [pltpu.VMEM((2, T // 2, c), F32) for c in parts]
            + [pltpu.VMEM((16, T), F32), pltpu.VMEM((3, R, 16, T), F32)]
            + [pltpu.VMEM((D, FF), BF16), pltpu.VMEM((D, FF), BF16), pltpu.VMEM((FF, D), BF16)]
            + [pltpu.VMEM((R * R * S, D), BF16), pltpu.VMEM((R * R * S, FF), BF16), pltpu.VMEM((T, D), F32)]
            + [pltpu.VMEM((2, D, tile), BF16), pltpu.VMEM((2, D, tile), BF16), pltpu.VMEM((2, tile, D), BF16)]
            + [dma((3,)), dma((2, 3))]
            + [dma((3,))] * 3 + [dma((3, R))]
            + [dma((3, HALVES)), dma((3, HALVES, R)), dma((3, HALVES)), dma((3, HALVES))]
            + [dma((3, HALVES)), dma((3, HALVES, R)), dma((3, HALVES)), dma((3, HALVES))] + [dma((3,))] * 2 + [dma((3, 2))]
            + [pltpu.SemaphoreType.REGULAR((3, HALVES))] * 2
        )
        y = pl.pallas_call(
            functools.partial(kernel, R, parts, tile, top, slots, names),
            out_shape=jax.ShapeDtypeStruct((T, D), BF16),
            in_specs=[vmem] * 4 + [any_space] * 6,
            out_specs=vmem,
            scratch_shapes=scratch,
            compiler_params=pltpu.CompilerParams(
                collective_id=0, has_side_effects=True, vmem_limit_bytes=67043328
            ),
            name="moe",
        )(x, expert, slot, gate, w_gate[0], w_up[0], w_down[0], s_gate, s_up, s_down)
        return y[None, None]

    tok = P("dp", "ep", None, None)
    exp = P("ep", None, None)
    rep = P(None, None)
    return jax.shard_map(
        step, mesh=mesh,
        in_specs=(tok, tok, tok, tok, exp, exp, exp, rep, rep, rep),
        out_specs=tok, check_vma=False,
    )
```

```python
import functools

import jax
import jax.numpy as jnp
from jax import lax
from jax.experimental import pallas as pl
from jax.experimental.pallas import tpu as pltpu
from jax.sharding import PartitionSpec as P

MESH = pl.DeviceIdType.MESH
BF16, F32 = jnp.bfloat16, jnp.float32
S = 16
HALVES = 2
SPAN = S * HALVES
ALL = slice(None)


def silu_mul(g, u):
    return (jax.nn.silu(g) * u).astype(BF16)


def kernel(R, parts, shared_tile, top, slots, names, *refs):
    (x_hbm, e_hbm, s_hbm, gate_hbm, wg_hbm, wu_hbm, wd_hbm, sg_hbm, su_hbm, sd_hbm, y_ref) = refs[:11]
    xa, g_buf, h_buf, z_buf, own = (refs[i:i + 3] for i in range(11, 26, 3))
    (x_ref, e_ref, s_ref, gate_ref, m_ref, meta, wg, wu, wd, zcat, hb, yacc, sgb, sub, sdb,
     in_sem, w_sem, sh_sem, m_s, m_r, a_s, a_r, b_s, b_r, c_s, c_r, c2_s, c2_r, b2_s, b2_r, a2_s, a2_r, ah_r, h_free, g_free) = refs[26:]
    dp_axis, ep_axis = names
    T = x_ref.shape[0]
    FF = wg.shape[1]
    KR = R * R * S
    dp, me = lax.axis_index(dp_axis), lax.axis_index(ep_axis)
    pos = (me // (R * R), lax.rem(me // R, R), lax.rem(me, R))
    unit = (R * R, R, 1)
    edges = [0]
    for c in parts:
        edges.append(edges[-1] + c)
    cols = [slice(edges[k], edges[k + 1]) for k in range(3)]

    order = sorted(range(3), key=lambda k: -parts[k])
    near = sorted(range(1, R), key=lambda r: (min(r, R - r), -r))
    ring4 = R == 4
    lo, hi = pl.ds(0, T // 2), pl.ds(T // 2, T // 2)

    def peer(axis, r):
        return me + (lax.rem(pos[axis] + r, R) - pos[axis]) * unit[axis]

    def zsl(k, a, b, c):
        i = [None] * 3
        i[k], i[(k + 1) % 3], i[(k + 2) % 3] = a, b, c
        return tuple(i)

    def hsl(k, a, b):
        return (a, b) if k < 2 else (b, a)

    def send(src, dst, s, r, axis, step):
        pltpu.make_async_remote_copy(
            src_ref=src, dst_ref=dst, send_sem=s, recv_sem=r,
            device_id=(dp, peer(axis, step)), device_id_type=MESH,
        ).start()

    def pend(ref, s, r):
        return pltpu.make_async_remote_copy(
            src_ref=ref, dst_ref=ref, send_sem=s, recv_sem=r,
            device_id=(dp, peer(0, 1)), device_id_type=MESH,
        )

    def whole(k, h):
        return g_buf[k].at[h, 1:R]

    n_sh = sg_hbm.shape[1] // shared_tile

    def sh_copies(j, slot):
        at = pl.ds(pl.multiple_of(j * shared_tile, shared_tile), shared_tile)
        return (
            pltpu.make_async_copy(sg_hbm.at[:, at], sgb.at[slot], sh_sem.at[slot, 0]),
            pltpu.make_async_copy(su_hbm.at[:, at], sub.at[slot], sh_sem.at[slot, 1]),
            pltpu.make_async_copy(sd_hbm.at[at], sdb.at[slot], sh_sem.at[slot, 2]),
        )

    in_copies = [
        pltpu.make_async_copy(src, dst, in_sem.at[i])
        for i, (src, dst) in enumerate(((x_hbm, x_ref), (e_hbm, e_ref), (s_hbm, s_ref), (gate_hbm, gate_ref)))
    ]
    for c in in_copies:
        c.start()

    def shared(j):
        slot = lax.rem(j, 2)
        for c in sh_copies(j, slot):
            c.wait()

        @pl.when(j + 1 < n_sh)
        def _():
            for c in sh_copies(j + 1, 1 - slot):
                c.start()

        g = jnp.dot(x_ref[...], sgb[slot], preferred_element_type=F32)
        u = jnp.dot(x_ref[...], sub[slot], preferred_element_type=F32)
        yacc[...] += jnp.dot(silu_mul(g, u), sdb[slot], preferred_element_type=F32)

    def slot_ids(k, h):
        row = lax.broadcasted_iota(jnp.int32, (KR, T), 0)
        rb, rc, s = row // (R * S), lax.rem(row // S, R), lax.rem(row, S)
        b, c = (k + 1) % 3, (k + 2) % 3
        e = pos[k] * unit[k] + lax.rem(rb + pos[b], R) * unit[b] + lax.rem(rc + pos[c], R) * unit[c]
        return (e * SPAN + s + h * S).astype(F32)

    def gather(k, h, ra, ids):
        hit = ids == meta[k, ra, 0:1, :]
        for j in range(1, top):
            hit = hit | (ids == meta[k, ra, j:j + 1, :])
        pick = jnp.where(hit, 1.0, 0.0).astype(BF16)
        rows = jnp.dot(pick, xa[k][ra], preferred_element_type=F32).astype(BF16)
        rows = rows.reshape(R, R, S, parts[k])
        g_buf[k][h, 1:R, :, ra] = rows[1:]
        z_buf[k][(h,) + zsl(k, ra, 0, 0)] = rows[0, 0]
        h_buf[k][(h, ALL) + hsl(k, ra, 0)] = rows[0, 1:]

    def send_b(k, h, ra):
        for rb in near:
            to = R - rb
            send(g_buf[k].at[h, rb, 1:R, ra], h_buf[k].at[(h, ALL) + hsl(k, ra, to)],
                 b_s.at[k, h], b_r.at[k, h, ra], (k + 1) % 3, rb)
            send(g_buf[k].at[h, rb, 0, ra], z_buf[k].at[(h,) + zsl(k, ra, to, 0)],
                 b_s.at[k, h], b_r.at[k, h, ra], (k + 1) % 3, rb)

    @jax.named_scope("relay_c")
    def relay_c(h, ra):
        for k in order:
            pend(g_buf[k].at[h, 1:R, :, 0], b_s.at[k, h], b_r.at[k, h, ra]).wait_recv()
            for rc in near:
                send(h_buf[k].at[(h, rc - 1) + hsl(k, ra, ALL)], z_buf[k].at[(h,) + zsl(k, ra, ALL, R - rc)],
                     c_s.at[k, h], c_r.at[k, h], (k + 2) % 3, rc)

    barrier = pltpu.get_barrier_semaphore()
    for axis in range(3):
        for r in range(1, R):
            pl.semaphore_signal(barrier, inc=1, device_id=(dp, peer(axis, r)), device_id_type=MESH)

    for c in sh_copies(0, 0):
        c.start()
    for c in in_copies[1:]:
        c.wait()
    m_ref[...] = jnp.zeros_like(m_ref)
    for j in range(top):
        m_ref[j:j + 1, :] = jnp.where(s_ref[j] < slots, e_ref[j] * SPAN + s_ref[j], -1).astype(F32)
        m_ref[8 + j:9 + j, :] = gate_ref[j].astype(BF16).astype(F32)
    in_copies[0].wait()
    with jax.named_scope("barrier"):
        pl.semaphore_wait(barrier, 3 * (R - 1))

    for k in order:
        for r in near:
            send(m_ref, meta.at[k, R - r], m_s.at[k], m_r.at[k], k, r)
    for r in near:
        if not ring4 or r != 2:
            for k in order:
                send(x_ref.at[:, cols[k]], xa[k].at[R - r], a_s.at[k], a_r.at[k, R - r], k, r)
    for k in range(3):
        meta[k, 0] = m_ref[...]
        xa[k][0] = x_ref[:, cols[k]]
    for k in order:
        gather(k, 0, 0, slot_ids(k, 0))
        send_b(k, 0, 0)
    yacc[...] = jnp.zeros_like(yacc)

    early = max(n_sh - R - 2, 0)
    pl.loop(0, early)(jax.named_scope("shared")(shared))

    @jax.named_scope("wait_a")
    def wait_a(k, ra):
        pend(xa[k].at[ra], a_s.at[k], a_r.at[k, ra]).wait_recv()

    @jax.named_scope("gather")
    def gather_all(h, ra, go):
        for k in order:
            gather(k, h, ra, slot_ids(k, h))
            if go:
                send_b(k, h, ra)

    for k in order:
        with jax.named_scope("wait_m"):
            pend(meta.at[k, 1:R], m_s.at[k], m_r.at[k]).wait_recv()
    if ring4:
        for k in order:
            wait_a(k, 3)
            send(xa[k].at[3, lo], xa[k].at[2, lo], a_s.at[k], a_r.at[k, 2], k, 1)
            wait_a(k, 1)
            send(xa[k].at[1, hi], xa[k].at[2, hi], a_s.at[k], a_r.at[k, 2], k, 3)
        seq = [0, 3, 1, 2]

        @pl.loop(0, 2)
        def _(i):
            gather_all(0, 3 - 2 * i, True)
    else:
        seq = list(range(R))
    pl.loop(early, n_sh - R)(jax.named_scope("shared")(shared))

    w_copies = [
        pltpu.make_async_copy(src, dst, w_sem.at[i])
        for i, (src, dst) in enumerate(((wg_hbm, wg), (wu_hbm, wu), (wd_hbm, wd)))
    ]
    for c in w_copies:
        c.start()

    for ra in [2] if ring4 else seq[1:]:
        for k in order:
            wait_a(k, ra)
        gather_all(0, ra, True)

    @pl.loop(0, R)
    def _(ra):
        gather_all(1, ra, False)

    @pl.loop(0, R)
    def _(i):
        with jax.named_scope("shared"):
            shared(n_sh - R + i)
        for step, ra in enumerate(seq):
            @pl.when(i == step)
            def _():
                relay_c(0, ra)
                for k in order:
                    send_b(k, 1, ra)

    for c in w_copies:
        c.wait()

    def send_c2(h, rx):
        for k in order:
            s, axis = c2_s.at[k, h], (k + 2) % 3
            z, hh, g = z_buf[k], h_buf[k], g_buf[k]
            if k == 0:
                for rc in near:
                    send(z.at[h, rx, 1:R, rc], hh.at[h, R - rc - 1, rx, 1:R], s, c2_r.at[k, h, R - rc], axis, rc)
                    send(z.at[h, rx, 0, rc], g.at[h, 0, R - rc, rx], s, c2_r.at[k, h, R - rc], axis, rc)
            elif k == 1:
                @pl.when(rx > 0)
                def _():
                    send(z.at[h, rx, :, 1:R], hh.at[h, R - rx - 1, :, 1:R], s, c2_r.at[k, h, R - rx], axis, rx)
                    send(z.at[h, rx, :, 0], g.at[h, 0, R - rx], s, c2_r.at[k, h, R - rx], axis, rx)
            else:
                @pl.when(rx > 0)
                def _():
                    for rc in near:
                        send(z.at[h, rx, rc], hh.at[h, R - rc - 1, rx], s, c2_r.at[k, h, R - rc], axis, rc)

                @pl.when(rx == 0)
                def _():
                    for rc in near:
                        send(z.at[h, rx, rc], g.at[h, 0, R - rc], s, c2_r.at[k, h, R - rc], axis, rc)

    def own_b2(h):
        for k in order:
            pl.semaphore_wait(g_free.at[k, h], R - 1)
            for rb in near:
                send(z_buf[k].at[(h,) + zsl(k, ALL, rb, 0)], g_buf[k].at[h, R - rb, 0],
                     b2_s.at[k, h], b2_r.at[k, h], (k + 1) % 3, rb)

    @jax.named_scope("relay_b2")
    def relay_b2(h):
        for ce in range(R - 1, 0, -1):
            for k in order:
                pend(g_buf[k].at[h, 1], c2_s.at[k, h], c2_r.at[k, h, ce]).wait_recv()
                for rb in near:
                    send(h_buf[k].at[(h, ce - 1) + hsl(k, ALL, rb)], g_buf[k].at[h, R - rb, ce],
                         b2_s.at[k, h], b2_r.at[k, h], (k + 1) % 3, rb)

    wide = [(n, min(512, FF - n)) for n in range(0, FF, 512)]

    @pl.loop(0, HALVES * R)
    def _(t):
        h, rx = t // R, lax.rem(t, R)

        @pl.when(rx == 0)
        @jax.named_scope("wait_c")
        def _():
            for k in range(3):
                pend(whole(k, h), c_s.at[k, h], c_r.at[k, h]).wait_recv()
            @pl.when(t == 0)
            def _():
                for k in range(3):
                    pend(xa[k].at[1:R], a_s.at[k], a2_r.at[k]).wait_send()

            for k in range(3):
                pend(whole(k, h), c_s.at[k, h], c_r.at[k, h]).wait_send()
                pend(whole(k, h), b_s.at[k, h], b_r.at[k, h]).wait_send()
                for free, axis in ((h_free, k + 2), (g_free, k + 1)):
                    for r in range(1, R):
                        pl.semaphore_signal(free.at[k, h], inc=1, device_id=(dp, peer(axis % 3, r)), device_id_type=MESH)

        @pl.when(t == 0)
        def _():
            for ra in seq[:R // 2]:
                relay_c(1, ra)

        with jax.named_scope("up"):
            for k in range(3):
                zcat[:, cols[k]] = z_buf[k][h, rx].reshape(KR, parts[k])
            for n, w in wide:
                g = jnp.dot(zcat[...], wg[:, n:n + w], preferred_element_type=F32)
                u = jnp.dot(zcat[...], wu[:, n:n + w], preferred_element_type=F32)
                hb[:, n:n + w] = silu_mul(g, u)
        with jax.named_scope("down"):
            for k in range(3):
                o = jnp.dot(hb[...], wd[:, cols[k]], preferred_element_type=F32)
                z_buf[k][h, rx] = o.astype(BF16).reshape(R, R, S, parts[k])

        @pl.when(rx == 0)
        def _():
            for k in range(3):
                pl.semaphore_wait(h_free.at[k, h], R - 1)

        send_c2(h, rx)

        @pl.when(t == 0)
        def _():
            for ra in seq[R // 2:]:
                relay_c(1, ra)

        @pl.when(rx == R - 1)
        def _():
            own_b2(h)

        @pl.when(t == R + R // 2 - 1)
        def _():
            relay_b2(0)

    def own_rows(k, h):
        g_buf[k][h, 0, 0] = z_buf[k][(h,) + zsl(k, ALL, 0, 0)]

    wide_w = HALVES * KR
    across = FF // wide_w

    def block(k, ra):
        i = k * R + ra
        return pl.ds(i // across * T, T), pl.ds(i % across * wide_w, wide_w)

    @jax.named_scope("weights")
    def build(k, ra):
        rows, columns = block(k, ra)
        for h in range(HALVES):
            ids = slot_ids(k, h)
            w = jnp.zeros((KR, T), F32)
            for j in range(top):
                w += jnp.where(ids == meta[k, ra, j:j + 1, :], meta[k, ra, 8 + j:9 + j, :], 0.0)
            wg[rows, pl.ds(columns.start + h * KR, KR)] = w.T.astype(BF16)

    def partial(k, ra):
        rows = g_buf[k][:, :, :, ra].reshape(wide_w, parts[k])
        return jnp.dot(wg[block(k, ra)], rows, preferred_element_type=F32)

    relay_b2(1)
    for k in order:
        for h in range(HALVES):
            own_rows(k, h)
    for ra in [2, 1, 3, 0] if ring4 else range(R):
        for k in order:
            build(k, ra)
    for k in order:
        with jax.named_scope("wait_b2"):
            pend(whole(k, 0), b2_s.at[k, 0], b2_r.at[k, 0]).wait_recv()
    for k in order:
        with jax.named_scope("wait_b2"):
            pend(whole(k, 1), b2_s.at[k, 1], b2_r.at[k, 1]).wait_recv()

    def ps(k, ra, at):
        beside = k == 2 and parts[0] + parts[2] <= FF
        row = ((0 if beside else k) * (R - 1) + ra - 1) * T + at.start
        left = parts[0] if beside else 0
        return wu.at[pl.ds(row, at.size), pl.ds(left, parts[k])]

    def send_a2(k, ra, at):
        send(ps(k, ra, at), xa[k].at[R - ra, at], a2_s.at[k], a2_r.at[k], k, ra)

    if ring4:
        for k in order:
            with jax.named_scope("weigh_far"):
                ps(k, 2, pl.ds(0, T))[...] = partial(k, 2).astype(BF16)
            send(ps(k, 2, lo), xa[k].at[2, lo], a2_s.at[k], ah_r.at[k, 0], k, 1)
            send(ps(k, 2, hi), xa[k].at[2, hi], a2_s.at[k], ah_r.at[k, 1], k, 3)
        for k in order:
            with jax.named_scope("weigh_near"):
                for i, (ra, now, later) in enumerate(((1, hi, lo), (3, lo, hi))):
                    p = partial(k, ra)
                    ps(k, ra, now)[...] = p[now.start:now.start + now.size].astype(BF16)
                    send_a2(k, ra, now)
                    own[k][i] = p[later.start:later.start + later.size]
        for k in order:
            for i, (ra, at) in enumerate(((1, lo), (3, hi))):
                with jax.named_scope("weigh_sum"):
                    pend(xa[k].at[2, at], a2_s.at[k], ah_r.at[k, i]).wait_recv()
                    ps(k, ra, at)[...] = (own[k][i] + xa[k][2, at].astype(F32)).astype(BF16)
                    send_a2(k, ra, at)
    else:
        for k in order:
            for ra in range(1, R):
                ps(k, ra, pl.ds(0, T))[...] = partial(k, ra).astype(BF16)
                send_a2(k, ra, pl.ds(0, T))
    senders = (1, 3) if ring4 else tuple(range(1, R))

    for k in order:
        with jax.named_scope("weigh_own"):
            yacc[:, cols[k]] += partial(k, 0)
    for k in order:
        with jax.named_scope("wait_a2"):
            pend(xa[k].at[0:len(senders)], a2_s.at[k], a2_r.at[k]).wait_recv()
        total = yacc[:, cols[k]]
        for ra in senders:
            total += xa[k][ra].astype(F32)
        y_ref[:, cols[k]] = total.astype(BF16)

    for k in range(3):
        pend(meta.at[k, 1:R], m_s.at[k], m_r.at[k]).wait_send()
        pend(xa[k].at[1:R], a2_s.at[k], a2_r.at[k]).wait_send()
        for h in range(HALVES):
            for s, r in ((c2_s, c2_r), (b2_s, b2_r)):
                pend(whole(k, h), s.at[k, h], r.at[k, h]).wait_send()


def split(d):
    tiles = d // 128
    low = tiles // 3
    sizes = [low, low, low]
    for i in range(tiles - 3 * low):
        sizes[2 - i] += 1
    return [128 * n for n in sizes]


def solution(mesh):
    names = ("dp", "ep")

    def step(x, expert, slot, gate, w_gate, w_up, w_down, s_gate, s_up, s_down):
        R = round(mesh.shape["ep"] ** (1 / 3))
        T, D = x.shape[2:]
        top, members = expert.shape[-1], mesh.shape["ep"]
        FF, SFF = w_gate.shape[-1], s_gate.shape[-1]
        slots = 5 * T * top // (4 * members)
        parts = split(D)
        x, (expert, slot, gate) = x[0, 0], (v[0].transpose(2, 0, 1) for v in (expert, slot, gate))
        any_space = pl.BlockSpec(memory_space=pl.ANY)
        vmem = pl.BlockSpec(memory_space=pltpu.VMEM)
        tile = min(256, SFF)
        dma = pltpu.SemaphoreType.DMA
        scratch = (
            [pltpu.VMEM((R, T, c), BF16) for c in parts]
            + [pltpu.VMEM((HALVES, R, R, R, S, c), BF16) for c in parts]
            + [pltpu.VMEM((HALVES, R - 1, R, R, S, c), BF16) for c in parts]
            + [pltpu.VMEM((HALVES, R, R, R, S, c), BF16) for c in parts]
            + [pltpu.VMEM((2, T // 2, c), F32) for c in parts]
            + [pltpu.VMEM((T, D), BF16), pltpu.VMEM((top, 1, T), jnp.int32), pltpu.VMEM((top, 1, T), jnp.int32),
               pltpu.VMEM((top, 1, T), F32)]
            + [pltpu.VMEM((16, T), F32), pltpu.VMEM((3, R, 16, T), F32)]
            + [pltpu.VMEM((D, FF), BF16), pltpu.VMEM((D, FF), BF16), pltpu.VMEM((FF, D), BF16)]
            + [pltpu.VMEM((R * R * S, D), BF16), pltpu.VMEM((R * R * S, FF), BF16), pltpu.VMEM((T, D), F32)]
            + [pltpu.VMEM((2, D, tile), BF16), pltpu.VMEM((2, D, tile), BF16), pltpu.VMEM((2, tile, D), BF16)]
            + [dma((4,)), dma((3,)), dma((2, 3))]
            + [dma((3,))] * 3 + [dma((3, R))]
            + [dma((3, HALVES)), dma((3, HALVES, R)), dma((3, HALVES)), dma((3, HALVES))]
            + [dma((3, HALVES)), dma((3, HALVES, R)), dma((3, HALVES)), dma((3, HALVES))] + [dma((3,))] * 2 + [dma((3, 2))]
            + [pltpu.SemaphoreType.REGULAR((3, HALVES))] * 2
        )
        y = pl.pallas_call(
            functools.partial(kernel, R, parts, tile, top, slots, names),
            out_shape=jax.ShapeDtypeStruct((T, D), BF16),
            in_specs=[any_space] * 10,
            out_specs=vmem,
            scratch_shapes=scratch,
            compiler_params=pltpu.CompilerParams(
                collective_id=0, has_side_effects=True, vmem_limit_bytes=67043328
            ),
            name="moe",
        )(x, expert, slot, gate, w_gate[0], w_up[0], w_down[0], s_gate, s_up, s_down)
        return y[None, None]

    tok = P("dp", "ep", None, None)
    exp = P("ep", None, None)
    rep = P(None, None)
    return jax.shard_map(
        step, mesh=mesh,
        in_specs=(tok, tok, tok, tok, exp, exp, exp, rep, rep, rep),
        out_specs=tok, check_vma=False,
    )
```

```python
import functools

import jax
import jax.numpy as jnp
from jax import lax
from jax.experimental import pallas as pl
from jax.experimental.pallas import tpu as pltpu
from jax.sharding import PartitionSpec as P

MESH = pl.DeviceIdType.MESH
BF16, F32 = jnp.bfloat16, jnp.float32
S = 16
HALVES = 2
SPAN = S * HALVES
ALL = slice(None)


def silu_mul(g, u):
    return (jax.nn.silu(g) * u).astype(BF16)


def kernel(R, parts, shared_tile, top, slots, names, *refs):
    (x_hbm, e_hbm, s_hbm, gate_hbm, wg_hbm, wu_hbm, wd_hbm, sg_hbm, su_hbm, sd_hbm, y_hbm) = refs[:11]
    xa, g_buf, h_buf, z_buf, own = (refs[i:i + 3] for i in range(11, 26, 3))
    (y_ref, x_ref, e_ref, s_ref, gate_ref, m_ref, meta, wg, wu, wd, zcat, hb, yacc, sgb, sub, sdb,
     out_sem, in_sem, w_sem, sh_sem, m_s, m_r, a_s, a_r, b_s, b_r, c_s, c_r, c2_s, c2_r, b2_s, b2_r, a2_s, a2_r, ah_r, h_free, g_free) = refs[26:]
    dp_axis, ep_axis = names
    T = x_ref.shape[0]
    FF = wg.shape[1]
    KR = R * R * S
    dp, me = lax.axis_index(dp_axis), lax.axis_index(ep_axis)
    pos = (me // (R * R), lax.rem(me // R, R), lax.rem(me, R))
    unit = (R * R, R, 1)
    edges = [0]
    for c in parts:
        edges.append(edges[-1] + c)
    cols = [slice(edges[k], edges[k + 1]) for k in range(3)]

    order = sorted(range(3), key=lambda k: -parts[k])
    near = sorted(range(1, R), key=lambda r: (min(r, R - r), -r))
    ring4 = R == 4
    back = (0, 2, 1)
    lo, hi = pl.ds(0, T // 2), pl.ds(T // 2, T // 2)

    def peer(axis, r):
        return me + (lax.rem(pos[axis] + r, R) - pos[axis]) * unit[axis]

    def zsl(k, a, b, c):
        i = [None] * 3
        i[k], i[(k + 1) % 3], i[(k + 2) % 3] = a, b, c
        return tuple(i)

    def hsl(k, a, b):
        return (a, b) if k < 2 else (b, a)

    def send(src, dst, s, r, axis, step):
        pltpu.make_async_remote_copy(
            src_ref=src, dst_ref=dst, send_sem=s, recv_sem=r,
            device_id=(dp, peer(axis, step)), device_id_type=MESH,
        ).start()

    def pend(ref, s, r):
        return pltpu.make_async_remote_copy(
            src_ref=ref, dst_ref=ref, send_sem=s, recv_sem=r,
            device_id=(dp, peer(0, 1)), device_id_type=MESH,
        )

    def whole(k, h):
        return g_buf[k].at[h, 1:R]

    n_sh = sg_hbm.shape[1] // shared_tile

    def sh_copies(j, slot):
        at = pl.ds(pl.multiple_of(j * shared_tile, shared_tile), shared_tile)
        return (
            pltpu.make_async_copy(sg_hbm.at[:, at], sgb.at[slot], sh_sem.at[slot, 0]),
            pltpu.make_async_copy(su_hbm.at[:, at], sub.at[slot], sh_sem.at[slot, 1]),
            pltpu.make_async_copy(sd_hbm.at[at], sdb.at[slot], sh_sem.at[slot, 2]),
        )

    in_copies = [
        pltpu.make_async_copy(src, dst, in_sem.at[i])
        for i, (src, dst) in enumerate(((x_hbm, x_ref), (e_hbm, e_ref), (s_hbm, s_ref), (gate_hbm, gate_ref)))
    ]
    for c in in_copies:
        c.start()

    def shared(j):
        slot = lax.rem(j, 2)
        for c in sh_copies(j, slot):
            c.wait()

        @pl.when(j + 1 < n_sh)
        def _():
            for c in sh_copies(j + 1, 1 - slot):
                c.start()

        g = jnp.dot(x_ref[...], sgb[slot], preferred_element_type=F32)
        u = jnp.dot(x_ref[...], sub[slot], preferred_element_type=F32)
        yacc[...] += jnp.dot(silu_mul(g, u), sdb[slot], preferred_element_type=F32)

    def slot_ids(k, h):
        row = lax.broadcasted_iota(jnp.int32, (KR, T), 0)
        rb, rc, s = row // (R * S), lax.rem(row // S, R), lax.rem(row, S)
        b, c = (k + 1) % 3, (k + 2) % 3
        e = pos[k] * unit[k] + lax.rem(rb + pos[b], R) * unit[b] + lax.rem(rc + pos[c], R) * unit[c]
        return (e * SPAN + s + h * S).astype(F32)

    def gather(k, h, ra, ids):
        hit = ids == meta[k, ra, 0:1, :]
        for j in range(1, top):
            hit = hit | (ids == meta[k, ra, j:j + 1, :])
        pick = jnp.where(hit, 1.0, 0.0).astype(BF16)
        rows = jnp.dot(pick, xa[k][ra], preferred_element_type=F32).astype(BF16)
        rows = rows.reshape(R, R, S, parts[k])
        g_buf[k][h, 1:R, :, ra] = rows[1:]
        z_buf[k][(h,) + zsl(k, ra, 0, 0)] = rows[0, 0]
        h_buf[k][(h, ALL) + hsl(k, ra, 0)] = rows[0, 1:]

    def send_b(k, h, ra):
        for rb in near:
            to = R - rb
            send(g_buf[k].at[h, rb, 1:R, ra], h_buf[k].at[(h, ALL) + hsl(k, ra, to)],
                 b_s.at[k, h], b_r.at[k, h, ra], (k + 1) % 3, rb)
            send(g_buf[k].at[h, rb, 0, ra], z_buf[k].at[(h,) + zsl(k, ra, to, 0)],
                 b_s.at[k, h], b_r.at[k, h, ra], (k + 1) % 3, rb)

    @jax.named_scope("relay_c")
    def relay_c(h, ra):
        for k in order:
            pend(g_buf[k].at[h, 1:R, :, 0], b_s.at[k, h], b_r.at[k, h, ra]).wait_recv()
            for rc in near:
                send(h_buf[k].at[(h, rc - 1) + hsl(k, ra, ALL)], z_buf[k].at[(h,) + zsl(k, ra, ALL, R - rc)],
                     c_s.at[k, h], c_r.at[k, h], (k + 2) % 3, rc)

    barrier = pltpu.get_barrier_semaphore()
    for axis in range(3):
        for r in range(1, R):
            pl.semaphore_signal(barrier, inc=1, device_id=(dp, peer(axis, r)), device_id_type=MESH)

    for c in sh_copies(0, 0):
        c.start()
    for c in in_copies[1:]:
        c.wait()
    m_ref[...] = jnp.zeros_like(m_ref)
    for j in range(top):
        m_ref[j:j + 1, :] = jnp.where(s_ref[j] < slots, e_ref[j] * SPAN + s_ref[j], -1).astype(F32)
        m_ref[8 + j:9 + j, :] = gate_ref[j].astype(BF16).astype(F32)
    in_copies[0].wait()
    with jax.named_scope("barrier"):
        pl.semaphore_wait(barrier, 3 * (R - 1))

    for k in order:
        for r in near:
            send(m_ref, meta.at[k, R - r], m_s.at[k], m_r.at[k], k, r)
    for r in near:
        if not ring4 or r != 2:
            for k in order:
                send(x_ref.at[:, cols[k]], xa[k].at[R - r], a_s.at[k], a_r.at[k, R - r], k, r)
    for k in range(3):
        meta[k, 0] = m_ref[...]
        xa[k][0] = x_ref[:, cols[k]]
    for k in order:
        gather(k, 0, 0, slot_ids(k, 0))
        send_b(k, 0, 0)
    yacc[...] = jnp.zeros_like(yacc)

    early = max(n_sh - R - 2, 0)
    pl.loop(0, early)(jax.named_scope("shared")(shared))

    @jax.named_scope("wait_a")
    def wait_a(k, ra):
        pend(xa[k].at[ra], a_s.at[k], a_r.at[k, ra]).wait_recv()

    @jax.named_scope("gather")
    def gather_all(h, ra, go):
        for k in order:
            gather(k, h, ra, slot_ids(k, h))
            if go:
                send_b(k, h, ra)

    for k in order:
        with jax.named_scope("wait_m"):
            pend(meta.at[k, 1:R], m_s.at[k], m_r.at[k]).wait_recv()
    if ring4:
        for k in order:
            wait_a(k, 3)
            send(xa[k].at[3, lo], xa[k].at[2, lo], a_s.at[k], a_r.at[k, 2], k, 1)
            wait_a(k, 1)
            send(xa[k].at[1, hi], xa[k].at[2, hi], a_s.at[k], a_r.at[k, 2], k, 3)
        seq = [0, 3, 1, 2]

        @pl.loop(0, 2)
        def _(i):
            gather_all(0, 3 - 2 * i, True)
    else:
        seq = list(range(R))
    pl.loop(early, n_sh - R)(jax.named_scope("shared")(shared))

    w_copies = [
        pltpu.make_async_copy(src, dst, w_sem.at[i])
        for i, (src, dst) in enumerate(((wg_hbm, wg), (wu_hbm, wu), (wd_hbm, wd)))
    ]
    for c in w_copies:
        c.start()

    for ra in [2] if ring4 else seq[1:]:
        for k in order:
            wait_a(k, ra)
        gather_all(0, ra, True)

    @pl.loop(0, R)
    def _(ra):
        gather_all(1, ra, False)

    @pl.loop(0, R)
    def _(i):
        with jax.named_scope("shared"):
            shared(n_sh - R + i)
        for step, ra in enumerate(seq):
            @pl.when(i == step)
            def _():
                relay_c(0, ra)
                for k in order:
                    send_b(k, 1, ra)

    for c in w_copies:
        c.wait()
    for ra in seq[:-1]:
        relay_c(1, ra)

    def send_c2(h, rx):
        for k in order:
            s, axis = c2_s.at[k, h], (back[k] + 2) % 3
            z, hh, g = z_buf[k], h_buf[k], g_buf[k]
            if back[k] == 0:
                for rc in near:
                    send(z.at[h, rx, 1:R, rc], hh.at[h, R - rc - 1, rx, 1:R], s, c2_r.at[k, h, R - rc], axis, rc)
                    send(z.at[h, rx, 0, rc], g.at[h, 0, R - rc, rx], s, c2_r.at[k, h, R - rc], axis, rc)
            elif back[k] == 1:
                @pl.when(rx > 0)
                def _():
                    send(z.at[h, rx, :, 1:R], hh.at[h, R - rx - 1, :, 1:R], s, c2_r.at[k, h, R - rx], axis, rx)
                    send(z.at[h, rx, :, 0], g.at[h, 0, R - rx], s, c2_r.at[k, h, R - rx], axis, rx)
            else:
                @pl.when(rx > 0)
                def _():
                    for rc in near:
                        send(z.at[h, rx, rc], hh.at[h, R - rc - 1, rx], s, c2_r.at[k, h, R - rc], axis, rc)

                @pl.when(rx == 0)
                def _():
                    for rc in near:
                        send(z.at[h, rx, rc], g.at[h, 0, R - rc], s, c2_r.at[k, h, R - rc], axis, rc)

    def own_b2(h):
        for k in order:
            pl.semaphore_wait(g_free.at[k, h], R - 1)
            for rb in near:
                send(z_buf[k].at[(h,) + zsl(back[k], ALL, rb, 0)], g_buf[k].at[h, R - rb, 0],
                     b2_s.at[k, h], b2_r.at[k, h], (back[k] + 1) % 3, rb)

    @jax.named_scope("relay_b2")
    def relay_b2(h):
        for ce in range(R - 1, 0, -1):
            for k in order:
                pend(g_buf[k].at[h, 1], c2_s.at[k, h], c2_r.at[k, h, ce]).wait_recv()
                for rb in near:
                    send(h_buf[k].at[(h, ce - 1) + hsl(back[k], ALL, rb)], g_buf[k].at[h, R - rb, ce],
                         b2_s.at[k, h], b2_r.at[k, h], (back[k] + 1) % 3, rb)

    wide = [(n, min(512, FF - n)) for n in range(0, FF, 512)]

    @pl.loop(0, HALVES * R)
    def _(t):
        h, rx = t // R, lax.rem(t, R)

        @pl.when(rx == 0)
        @jax.named_scope("wait_c")
        def _():
            for k in range(3):
                pend(whole(k, h), c_s.at[k, h], c_r.at[k, h]).wait_recv()
            @pl.when(t == 0)
            def _():
                for k in range(3):
                    pend(xa[k].at[1:R], a_s.at[k], a2_r.at[k]).wait_send()

            for k in range(3):
                pend(whole(k, h), c_s.at[k, h], c_r.at[k, h]).wait_send()
                pend(whole(k, h), b_s.at[k, h], b_r.at[k, h]).wait_send()
                for free, axis in ((h_free, back[k] + 2), (g_free, back[k] + 1)):
                    for r in range(1, R):
                        pl.semaphore_signal(free.at[k, h], inc=1, device_id=(dp, peer(axis % 3, r)), device_id_type=MESH)

        with jax.named_scope("up"):
            for k in range(3):
                zcat[:, cols[k]] = z_buf[k][h, rx].reshape(KR, parts[k])
            for n, w in wide:
                g = jnp.dot(zcat[...], wg[:, n:n + w], preferred_element_type=F32)
                u = jnp.dot(zcat[...], wu[:, n:n + w], preferred_element_type=F32)
                hb[:, n:n + w] = silu_mul(g, u)
        with jax.named_scope("down"):
            for k in range(3):
                o = jnp.dot(hb[...], wd[:, cols[k]], preferred_element_type=F32)
                z_buf[k][h, rx] = o.astype(BF16).reshape(R, R, S, parts[k])

        @pl.when(rx == 0)
        def _():
            for k in range(3):
                pl.semaphore_wait(h_free.at[k, h], R - 1)

        send_c2(h, rx)

        @pl.when(t == 0)
        def _():
            relay_c(1, seq[-1])

        @pl.when(rx == R - 1)
        def _():
            own_b2(h)

        @pl.when(t == R)
        def _():
            relay_b2(0)

    def own_rows(k, h):
        g_buf[k][h, 0, 0] = z_buf[k][(h,) + zsl(back[k], ALL, 0, 0)]

    wide_w = HALVES * KR
    across = FF // wide_w

    def block(k, ra):
        i = k * R + ra
        return pl.ds(i // across * T, T), pl.ds(i % across * wide_w, wide_w)

    @jax.named_scope("weights")
    def build(k, ra):
        rows, columns = block(k, ra)
        for h in range(HALVES):
            ids = slot_ids(back[k], h)
            w = jnp.zeros((KR, T), F32)
            for j in range(top):
                w += jnp.where(ids == meta[back[k], ra, j:j + 1, :], meta[back[k], ra, 8 + j:9 + j, :], 0.0)
            wg[rows, pl.ds(columns.start + h * KR, KR)] = w.T.astype(BF16)

    def partial(k, ra):
        rows = g_buf[k][:, :, :, ra].reshape(wide_w, parts[k])
        return jnp.dot(wg[block(k, ra)], rows, preferred_element_type=F32)

    relay_b2(1)
    for k in order:
        for h in range(HALVES):
            own_rows(k, h)
    for ra in [2, 1, 3, 0] if ring4 else range(R):
        for k in order:
            build(k, ra)
    for k in order:
        with jax.named_scope("wait_b2"):
            pend(whole(k, 0), b2_s.at[k, 0], b2_r.at[k, 0]).wait_recv()
    for k in order:
        with jax.named_scope("wait_b2"):
            pend(whole(k, 1), b2_s.at[k, 1], b2_r.at[k, 1]).wait_recv()

    def ps(k, ra, at):
        beside = k == 2 and parts[0] + parts[2] <= FF
        row = ((0 if beside else k) * (R - 1) + ra - 1) * T + at.start
        left = parts[0] if beside else 0
        return wu.at[pl.ds(row, at.size), pl.ds(left, parts[k])]

    def send_a2(k, ra, at):
        send(ps(k, ra, at), xa[k].at[R - ra, at], a2_s.at[k], a2_r.at[k], back[k], ra)

    if ring4:
        for k in order:
            with jax.named_scope("weigh_far"):
                ps(k, 2, pl.ds(0, T))[...] = partial(k, 2).astype(BF16)
            send(ps(k, 2, lo), xa[k].at[2, lo], a2_s.at[k], ah_r.at[k, 0], back[k], 1)
            send(ps(k, 2, hi), xa[k].at[2, hi], a2_s.at[k], ah_r.at[k, 1], back[k], 3)
        for k in order:
            with jax.named_scope("weigh_near"):
                for i, (ra, now, later) in enumerate(((1, hi, lo), (3, lo, hi))):
                    p = partial(k, ra)
                    ps(k, ra, now)[...] = p[now.start:now.start + now.size].astype(BF16)
                    send_a2(k, ra, now)
                    own[k][i] = p[later.start:later.start + later.size]
        for k in order:
            for i, (ra, at) in enumerate(((1, lo), (3, hi))):
                with jax.named_scope("weigh_sum"):
                    pend(xa[k].at[2, at], a2_s.at[k], ah_r.at[k, i]).wait_recv()
                    ps(k, ra, at)[...] = (own[k][i] + xa[k][2, at].astype(F32)).astype(BF16)
                    send_a2(k, ra, at)
    else:
        for k in order:
            for ra in range(1, R):
                ps(k, ra, pl.ds(0, T))[...] = partial(k, ra).astype(BF16)
                send_a2(k, ra, pl.ds(0, T))
    senders = (1, 3) if ring4 else tuple(range(1, R))

    for k in order:
        with jax.named_scope("weigh_own"):
            yacc[:, cols[k]] += partial(k, 0)
    for k in order:
        with jax.named_scope("wait_a2"):
            pend(xa[k].at[0:len(senders)], a2_s.at[k], a2_r.at[k]).wait_recv()
        total = yacc[:, cols[k]]
        for ra in senders:
            total += xa[k][ra].astype(F32)
        y_ref[:, cols[k]] = total.astype(BF16)
        pltpu.make_async_copy(y_ref.at[:, cols[k]], y_hbm.at[:, cols[k]], out_sem.at[k]).start()

    for k in range(3):
        pltpu.make_async_copy(y_ref.at[:, cols[k]], y_hbm.at[:, cols[k]], out_sem.at[k]).wait()
        pend(meta.at[k, 1:R], m_s.at[k], m_r.at[k]).wait_send()
        pend(xa[k].at[1:R], a2_s.at[k], a2_r.at[k]).wait_send()
        for h in range(HALVES):
            for s, r in ((c2_s, c2_r), (b2_s, b2_r)):
                pend(whole(k, h), s.at[k, h], r.at[k, h]).wait_send()


def hand_on(pieces, src, dst, held, in_sem, out_sem):
    n = src.shape[0] // pieces
    rows = [pl.ds(i * n, n) for i in range(pieces)]
    into = [pltpu.make_async_copy(src.at[r], held.at[r], in_sem.at[i]) for i, r in enumerate(rows)]
    out = [pltpu.make_async_copy(held.at[r], dst.at[r], out_sem.at[i]) for i, r in enumerate(rows)]
    for c in into:
        c.start()
    for a, b in zip(into, out):
        a.wait()
        b.start()
    for c in out:
        c.wait()


def split(d):
    tiles = d // 128
    low = tiles // 3
    sizes = [low, low, low]
    for i in range(tiles - 3 * low):
        sizes[2 - i] += 1
    return [128 * n for n in sizes]


def solution(mesh):
    names = ("dp", "ep")

    def step(x, expert, slot, gate, w_gate, w_up, w_down, s_gate, s_up, s_down):
        R = round(mesh.shape["ep"] ** (1 / 3))
        T, D = x.shape[2:]
        top, members = expert.shape[-1], mesh.shape["ep"]
        FF, SFF = w_gate.shape[-1], s_gate.shape[-1]
        slots = 5 * T * top // (4 * members)
        parts = split(D)
        x, (expert, slot, gate) = x[0, 0], (v[0].transpose(2, 0, 1) for v in (expert, slot, gate))
        any_space = pl.BlockSpec(memory_space=pl.ANY)
        tile = min(256, SFF)
        dma = pltpu.SemaphoreType.DMA
        scratch = (
            [pltpu.VMEM((R, T, c), BF16) for c in parts]
            + [pltpu.VMEM((HALVES, R, R, R, S, c), BF16) for c in parts]
            + [pltpu.VMEM((HALVES, R - 1, R, R, S, c), BF16) for c in parts]
            + [pltpu.VMEM((HALVES, R, R, R, S, c), BF16) for c in parts]
            + [pltpu.VMEM((2, T // 2, c), F32) for c in parts]
            + [pltpu.VMEM((T, D), BF16), pltpu.VMEM((T, D), BF16), pltpu.VMEM((top, 1, T), jnp.int32), pltpu.VMEM((top, 1, T), jnp.int32),
               pltpu.VMEM((top, 1, T), F32)]
            + [pltpu.VMEM((16, T), F32), pltpu.VMEM((3, R, 16, T), F32)]
            + [pltpu.VMEM((D, FF), BF16), pltpu.VMEM((D, FF), BF16), pltpu.VMEM((FF, D), BF16)]
            + [pltpu.VMEM((R * R * S, D), BF16), pltpu.VMEM((R * R * S, FF), BF16), pltpu.VMEM((T, D), F32)]
            + [pltpu.VMEM((2, D, tile), BF16), pltpu.VMEM((2, D, tile), BF16), pltpu.VMEM((2, tile, D), BF16)]
            + [dma((3,)), dma((4,)), dma((3,)), dma((2, 3))]
            + [dma((3,))] * 3 + [dma((3, R))]
            + [dma((3, HALVES)), dma((3, HALVES, R)), dma((3, HALVES)), dma((3, HALVES))]
            + [dma((3, HALVES)), dma((3, HALVES, R)), dma((3, HALVES)), dma((3, HALVES))] + [dma((3,))] * 2 + [dma((3, 2))]
            + [pltpu.SemaphoreType.REGULAR((3, HALVES))] * 2
        )
        y = pl.pallas_call(
            functools.partial(kernel, R, parts, tile, top, slots, names),
            out_shape=jax.ShapeDtypeStruct((T, D), BF16),
            in_specs=[any_space] * 10,
            out_specs=any_space,
            scratch_shapes=scratch,
            compiler_params=pltpu.CompilerParams(
                collective_id=0, has_side_effects=True, vmem_limit_bytes=67043328
            ),
            name="moe",
        )(x, expert, slot, gate, w_gate[0], w_up[0], w_down[0], s_gate, s_up, s_down)
        pieces = 8
        y = pl.pallas_call(
            functools.partial(hand_on, pieces),
            out_shape=jax.ShapeDtypeStruct((T, D), BF16),
            in_specs=[any_space],
            out_specs=any_space,
            scratch_shapes=[pltpu.VMEM((T, D), BF16), dma((pieces,)), dma((pieces,))],
            name="hand_on",
        )(y)
        return y[None, None]

    tok = P("dp", "ep", None, None)
    exp = P("ep", None, None)
    rep = P(None, None)
    return jax.shard_map(
        step, mesh=mesh,
        in_specs=(tok, tok, tok, tok, exp, exp, exp, rep, rep, rep),
        out_specs=tok, check_vma=False,
    )
```

```python
import functools

import jax
import jax.numpy as jnp
from jax import lax
from jax.experimental import pallas as pl
from jax.experimental.pallas import tpu as pltpu
from jax.sharding import PartitionSpec as P

MESH = pl.DeviceIdType.MESH
BF16, F32 = jnp.bfloat16, jnp.float32
S = 16
HALVES = 2
SPAN = S * HALVES
ALL = slice(None)


def silu_mul(g, u):
    return (jax.nn.silu(g) * u).astype(BF16)


def kernel(R, parts, shared_tile, top, slots, names, *refs):
    (x_hbm, e_hbm, s_hbm, gate_hbm, wg_hbm, wu_hbm, wd_hbm, sg_hbm, su_hbm, sd_hbm, y_hbm) = refs[:11]
    xa, g_buf, h_buf, z_buf, own = (refs[i:i + 3] for i in range(11, 26, 3))
    (y_ref, x_ref, e_ref, s_ref, gate_ref, m_ref, meta, wg, wu, wd, zcat, hb, yacc, sgb, sub, sdb,
     out_sem, in_sem, w_sem, sh_sem, m_s, m_r, a_s, a_r, b_s, b_r, c_s, c_r, c2_s, c2_r, b2_s, b2_r, a2_s, a2_r, ah_r, h_free, g_free) = refs[26:]
    dp_axis, ep_axis = names
    T = x_ref.shape[0]
    FF = wg.shape[1]
    KR = R * R * S
    dp, me = lax.axis_index(dp_axis), lax.axis_index(ep_axis)
    pos = (me // (R * R), lax.rem(me // R, R), lax.rem(me, R))
    unit = (R * R, R, 1)
    edges = [0]
    for c in parts:
        edges.append(edges[-1] + c)
    cols = [slice(edges[k], edges[k + 1]) for k in range(3)]

    order = sorted(range(3), key=lambda k: -parts[k])
    near = sorted(range(1, R), key=lambda r: (min(r, R - r), -r))
    ring4 = R == 4
    back = (0, 2, 1)
    lo, hi = pl.ds(0, T // 2), pl.ds(T // 2, T // 2)

    def peer(axis, r):
        return me + (lax.rem(pos[axis] + r, R) - pos[axis]) * unit[axis]

    def zsl(k, a, b, c):
        i = [None] * 3
        i[k], i[(k + 1) % 3], i[(k + 2) % 3] = a, b, c
        return tuple(i)

    def hsl(k, a, b):
        return (a, b) if k < 2 else (b, a)

    def send(src, dst, s, r, axis, step):
        pltpu.make_async_remote_copy(
            src_ref=src, dst_ref=dst, send_sem=s, recv_sem=r,
            device_id=(dp, peer(axis, step)), device_id_type=MESH,
        ).start()

    def pend(ref, s, r):
        return pltpu.make_async_remote_copy(
            src_ref=ref, dst_ref=ref, send_sem=s, recv_sem=r,
            device_id=(dp, peer(0, 1)), device_id_type=MESH,
        )

    def whole(k, h):
        return g_buf[k].at[h, 1:R]

    n_sh = sg_hbm.shape[1] // shared_tile

    def sh_copies(j, slot):
        at = pl.ds(pl.multiple_of(j * shared_tile, shared_tile), shared_tile)
        return (
            pltpu.make_async_copy(sg_hbm.at[:, at], sgb.at[slot], sh_sem.at[slot, 0]),
            pltpu.make_async_copy(su_hbm.at[:, at], sub.at[slot], sh_sem.at[slot, 1]),
            pltpu.make_async_copy(sd_hbm.at[at], sdb.at[slot], sh_sem.at[slot, 2]),
        )

    in_copies = [
        pltpu.make_async_copy(src, dst, in_sem.at[i])
        for i, (src, dst) in enumerate(((x_hbm, x_ref), (e_hbm, e_ref), (s_hbm, s_ref), (gate_hbm, gate_ref)))
    ]
    for c in in_copies:
        c.start()

    def shared(j):
        slot = lax.rem(j, 2)
        for c in sh_copies(j, slot):
            c.wait()

        @pl.when(j + 1 < n_sh)
        def _():
            for c in sh_copies(j + 1, 1 - slot):
                c.start()

        g = jnp.dot(x_ref[...], sgb[slot], preferred_element_type=F32)
        u = jnp.dot(x_ref[...], sub[slot], preferred_element_type=F32)
        yacc[...] += jnp.dot(silu_mul(g, u), sdb[slot], preferred_element_type=F32)

    def slot_ids(k, h):
        row = lax.broadcasted_iota(jnp.int32, (KR, T), 0)
        rb, rc, s = row // (R * S), lax.rem(row // S, R), lax.rem(row, S)
        b, c = (k + 1) % 3, (k + 2) % 3
        e = pos[k] * unit[k] + lax.rem(rb + pos[b], R) * unit[b] + lax.rem(rc + pos[c], R) * unit[c]
        return (e * SPAN + s + h * S).astype(F32)

    def gather(k, h, ra, ids):
        hit = ids == meta[k, ra, 0:1, :]
        for j in range(1, top):
            hit = hit | (ids == meta[k, ra, j:j + 1, :])
        pick = jnp.where(hit, 1.0, 0.0).astype(BF16)
        rows = jnp.dot(pick, xa[k][ra], preferred_element_type=F32).astype(BF16)
        rows = rows.reshape(R, R, S, parts[k])
        g_buf[k][h, 1:R, :, ra] = rows[1:]
        z_buf[k][(h,) + zsl(k, ra, 0, 0)] = rows[0, 0]
        h_buf[k][(h, ALL) + hsl(k, ra, 0)] = rows[0, 1:]

    def send_b(k, h, ra):
        for rb in near:
            to = R - rb
            send(g_buf[k].at[h, rb, 1:R, ra], h_buf[k].at[(h, ALL) + hsl(k, ra, to)],
                 b_s.at[k, h], b_r.at[k, h, ra], (k + 1) % 3, rb)
            send(g_buf[k].at[h, rb, 0, ra], z_buf[k].at[(h,) + zsl(k, ra, to, 0)],
                 b_s.at[k, h], b_r.at[k, h, ra], (k + 1) % 3, rb)

    @jax.named_scope("relay_c")
    def relay_c(h, ra):
        for k in order:
            pend(g_buf[k].at[h, 1:R, :, 0], b_s.at[k, h], b_r.at[k, h, ra]).wait_recv()
            for rc in near:
                send(h_buf[k].at[(h, rc - 1) + hsl(k, ra, ALL)], z_buf[k].at[(h,) + zsl(k, ra, ALL, R - rc)],
                     c_s.at[k, h], c_r.at[k, h], (k + 2) % 3, rc)

    barrier = pltpu.get_barrier_semaphore()
    for axis in range(3):
        for r in range(1, R):
            pl.semaphore_signal(barrier, inc=1, device_id=(dp, peer(axis, r)), device_id_type=MESH)

    for c in sh_copies(0, 0):
        c.start()
    for c in in_copies[1:]:
        c.wait()
    m_ref[...] = jnp.zeros_like(m_ref)
    for j in range(top):
        m_ref[j:j + 1, :] = jnp.where(s_ref[j] < slots, e_ref[j] * SPAN + s_ref[j], -1).astype(F32)
        m_ref[8 + j:9 + j, :] = gate_ref[j].astype(BF16).astype(F32)
    in_copies[0].wait()
    with jax.named_scope("barrier"):
        pl.semaphore_wait(barrier, 3 * (R - 1))

    for k in order:
        for r in near:
            send(m_ref, meta.at[k, R - r], m_s.at[k], m_r.at[k], k, r)
    halves = {1: (lo, hi), 3: (hi, lo)} if ring4 else {r: (lo, hi) for r in near}
    for i in range(2):
        for r in halves:
            at = halves[r][i]
            for k in order:
                send(x_ref.at[at, cols[k]], xa[k].at[R - r, at], a_s.at[k], a_r.at[k, R - r, i], k, r)
    for k in range(3):
        meta[k, 0] = m_ref[...]
        xa[k][0] = x_ref[:, cols[k]]
    yacc[...] = jnp.zeros_like(yacc)
    for k in order:
        gather(k, 0, 0, slot_ids(k, 0))

    late = 2 * R - 1
    early = max(n_sh - late, 0)

    @jax.named_scope("wait_a")
    def wait_a(k, ra, i):
        pend(xa[k].at[ra, lo], a_s.at[k], a_r.at[k, ra, i]).wait_recv()

    @jax.named_scope("gather")
    def gather_all(h, ra, go):
        for k in order:
            gather(k, h, ra, slot_ids(k, h))
            if go:
                send_b(k, h, ra)

    pl.loop(0, early // 2)(jax.named_scope("shared")(shared))
    if ring4:
        seq = [0, 3, 1, 2]
        for k in order:
            wait_a(k, 3, 0)
            send(xa[k].at[3, lo], xa[k].at[2, lo], a_s.at[k], a_r.at[k, 2, 0], k, 1)
            wait_a(k, 1, 0)
            send(xa[k].at[1, hi], xa[k].at[2, hi], a_s.at[k], a_r.at[k, 2, 1], k, 3)
    else:
        seq = list(range(R))
        for r in near:
            for k in order:
                wait_a(k, r, 0)
    for k in order:
        send_b(k, 0, 0)
    pl.loop(early // 2, early)(jax.named_scope("shared")(shared))
    for k in order:
        with jax.named_scope("wait_m"):
            pend(meta.at[k, 1:R], m_s.at[k], m_r.at[k]).wait_recv()
    for ra in seq[1:]:
        for k in order:
            if ring4 and ra == 2:
                wait_a(k, ra, 0)
            wait_a(k, ra, 1)
        gather_all(0, ra, True)

    w_copies = [
        pltpu.make_async_copy(src, dst, w_sem.at[i])
        for i, (src, dst) in enumerate(((wg_hbm, wg), (wu_hbm, wu), (wd_hbm, wd)))
    ]
    for c in w_copies:
        c.start()

    @pl.loop(0, R)
    def _(ra):
        gather_all(1, ra, False)

    @pl.loop(0, late)
    def _(i):
        for step, ra in enumerate(seq):
            @pl.when(i == 2 * step)
            def _():
                relay_c(0, ra)
                for k in order:
                    send_b(k, 1, ra)

        @pl.when(early + i < n_sh)
        @jax.named_scope("shared")
        def _():
            shared(early + i)

    for c in w_copies:
        c.wait()
    for ra in seq[:-1]:
        relay_c(1, ra)

    def send_c2(h, rx):
        for k in order:
            s, axis = c2_s.at[k, h], (back[k] + 2) % 3
            z, hh, g = z_buf[k], h_buf[k], g_buf[k]
            if back[k] == 0:
                for rc in near:
                    send(z.at[h, rx, 1:R, rc], hh.at[h, R - rc - 1, rx, 1:R], s, c2_r.at[k, h, R - rc], axis, rc)
                    send(z.at[h, rx, 0, rc], g.at[h, 0, R - rc, rx], s, c2_r.at[k, h, R - rc], axis, rc)
            elif back[k] == 1:
                @pl.when(rx > 0)
                def _():
                    send(z.at[h, rx, :, 1:R], hh.at[h, R - rx - 1, :, 1:R], s, c2_r.at[k, h, R - rx], axis, rx)
                    send(z.at[h, rx, :, 0], g.at[h, 0, R - rx], s, c2_r.at[k, h, R - rx], axis, rx)
            else:
                @pl.when(rx > 0)
                def _():
                    for rc in near:
                        send(z.at[h, rx, rc], hh.at[h, R - rc - 1, rx], s, c2_r.at[k, h, R - rc], axis, rc)

                @pl.when(rx == 0)
                def _():
                    for rc in near:
                        send(z.at[h, rx, rc], g.at[h, 0, R - rc], s, c2_r.at[k, h, R - rc], axis, rc)

    def own_b2(h):
        for k in order:
            pl.semaphore_wait(g_free.at[k, h], R - 1)
            for rb in near:
                send(z_buf[k].at[(h,) + zsl(back[k], ALL, rb, 0)], g_buf[k].at[h, R - rb, 0],
                     b2_s.at[k, h], b2_r.at[k, h], (back[k] + 1) % 3, rb)

    @jax.named_scope("relay_b2")
    def relay_b2(h):
        for ce in range(R - 1, 0, -1):
            for k in order:
                pend(g_buf[k].at[h, 1], c2_s.at[k, h], c2_r.at[k, h, ce]).wait_recv()
                for rb in near:
                    send(h_buf[k].at[(h, ce - 1) + hsl(back[k], ALL, rb)], g_buf[k].at[h, R - rb, ce],
                         b2_s.at[k, h], b2_r.at[k, h], (back[k] + 1) % 3, rb)

    wide = [(n, min(512, FF - n)) for n in range(0, FF, 512)]

    @pl.loop(0, HALVES * R)
    def _(t):
        h, rx = t // R, lax.rem(t, R)

        @pl.when(rx == 0)
        @jax.named_scope("wait_c")
        def _():
            for k in range(3):
                pend(whole(k, h), c_s.at[k, h], c_r.at[k, h]).wait_recv()
            @pl.when(t == 0)
            def _():
                for k in range(3):
                    pend(xa[k].at[1:R], a_s.at[k], a2_r.at[k]).wait_send()

            for k in range(3):
                pend(whole(k, h), c_s.at[k, h], c_r.at[k, h]).wait_send()
                pend(whole(k, h), b_s.at[k, h], b_r.at[k, h]).wait_send()
                for free, axis in ((h_free, back[k] + 2), (g_free, back[k] + 1)):
                    for r in range(1, R):
                        pl.semaphore_signal(free.at[k, h], inc=1, device_id=(dp, peer(axis % 3, r)), device_id_type=MESH)

        with jax.named_scope("up"):
            for k in range(3):
                zcat[:, cols[k]] = z_buf[k][h, rx].reshape(KR, parts[k])
            for n, w in wide:
                g = jnp.dot(zcat[...], wg[:, n:n + w], preferred_element_type=F32)
                u = jnp.dot(zcat[...], wu[:, n:n + w], preferred_element_type=F32)
                hb[:, n:n + w] = silu_mul(g, u)
        with jax.named_scope("down"):
            for k in range(3):
                o = jnp.dot(hb[...], wd[:, cols[k]], preferred_element_type=F32)
                z_buf[k][h, rx] = o.astype(BF16).reshape(R, R, S, parts[k])

        @pl.when(rx == 0)
        def _():
            for k in range(3):
                pl.semaphore_wait(h_free.at[k, h], R - 1)

        send_c2(h, rx)

        @pl.when(t == 0)
        def _():
            relay_c(1, seq[-1])

        @pl.when(rx == R - 1)
        def _():
            own_b2(h)

        @pl.when(t == R + R // 2 - 1)
        def _():
            relay_b2(0)

    def own_rows(k, h):
        g_buf[k][h, 0, 0] = z_buf[k][(h,) + zsl(back[k], ALL, 0, 0)]

    wide_w = HALVES * KR
    across = FF // wide_w

    def block(k, ra):
        i = k * R + ra
        return pl.ds(i // across * T, T), pl.ds(i % across * wide_w, wide_w)

    @jax.named_scope("weights")
    def build(k, ra):
        rows, columns = block(k, ra)
        for h in range(HALVES):
            ids = slot_ids(back[k], h)
            w = jnp.zeros((KR, T), F32)
            for j in range(top):
                w += jnp.where(ids == meta[back[k], ra, j:j + 1, :], meta[back[k], ra, 8 + j:9 + j, :], 0.0)
            wg[rows, pl.ds(columns.start + h * KR, KR)] = w.T.astype(BF16)

    def partial(k, ra):
        rows = g_buf[k][:, :, :, ra].reshape(wide_w, parts[k])
        return jnp.dot(wg[block(k, ra)], rows, preferred_element_type=F32)

    relay_b2(1)
    for k in order:
        for h in range(HALVES):
            own_rows(k, h)
    for ra in [2, 1, 3, 0] if ring4 else range(R):
        for k in order:
            build(k, ra)
    for k in order:
        with jax.named_scope("wait_b2"):
            pend(whole(k, 0), b2_s.at[k, 0], b2_r.at[k, 0]).wait_recv()
    for k in order:
        with jax.named_scope("wait_b2"):
            pend(whole(k, 1), b2_s.at[k, 1], b2_r.at[k, 1]).wait_recv()

    def ps(k, ra, at):
        beside = k == 2 and parts[0] + parts[2] <= FF
        row = ((0 if beside else k) * (R - 1) + ra - 1) * T + at.start
        left = parts[0] if beside else 0
        return wu.at[pl.ds(row, at.size), pl.ds(left, parts[k])]

    def send_a2(k, ra, at):
        send(ps(k, ra, at), xa[k].at[R - ra, at], a2_s.at[k], a2_r.at[k], back[k], ra)

    if ring4:
        for k in order:
            with jax.named_scope("weigh_far"):
                ps(k, 2, pl.ds(0, T))[...] = partial(k, 2).astype(BF16)
            send(ps(k, 2, lo), xa[k].at[2, lo], a2_s.at[k], ah_r.at[k, 0], back[k], 1)
            send(ps(k, 2, hi), xa[k].at[2, hi], a2_s.at[k], ah_r.at[k, 1], back[k], 3)
        for k in order:
            with jax.named_scope("weigh_near"):
                for i, (ra, now, later) in enumerate(((1, hi, lo), (3, lo, hi))):
                    p = partial(k, ra)
                    ps(k, ra, now)[...] = p[now.start:now.start + now.size].astype(BF16)
                    send_a2(k, ra, now)
                    own[k][i] = p[later.start:later.start + later.size]
        for k in order:
            for i, (ra, at) in enumerate(((1, lo), (3, hi))):
                with jax.named_scope("weigh_sum"):
                    pend(xa[k].at[2, at], a2_s.at[k], ah_r.at[k, i]).wait_recv()
                    ps(k, ra, at)[...] = (own[k][i] + xa[k][2, at].astype(F32)).astype(BF16)
                    send_a2(k, ra, at)
    else:
        for k in order:
            for ra in range(1, R):
                ps(k, ra, pl.ds(0, T))[...] = partial(k, ra).astype(BF16)
                send_a2(k, ra, pl.ds(0, T))
    senders = (1, 3) if ring4 else tuple(range(1, R))

    for k in order:
        with jax.named_scope("weigh_own"):
            yacc[:, cols[k]] += partial(k, 0)
    for k in order:
        with jax.named_scope("wait_a2"):
            pend(xa[k].at[0:len(senders)], a2_s.at[k], a2_r.at[k]).wait_recv()
        total = yacc[:, cols[k]]
        for ra in senders:
            total += xa[k][ra].astype(F32)
        y_ref[:, cols[k]] = total.astype(BF16)
        pltpu.make_async_copy(y_ref.at[:, cols[k]], y_hbm.at[:, cols[k]], out_sem.at[k]).start()

    for k in range(3):
        pltpu.make_async_copy(y_ref.at[:, cols[k]], y_hbm.at[:, cols[k]], out_sem.at[k]).wait()
        pend(meta.at[k, 1:R], m_s.at[k], m_r.at[k]).wait_send()
        pend(xa[k].at[1:R], a2_s.at[k], a2_r.at[k]).wait_send()
        for h in range(HALVES):
            for s, r in ((c2_s, c2_r), (b2_s, b2_r)):
                pend(whole(k, h), s.at[k, h], r.at[k, h]).wait_send()


def hand_on(pieces, src, dst, held, in_sem, out_sem):
    n = src.shape[0] // pieces
    rows = [pl.ds(i * n, n) for i in range(pieces)]
    into = [pltpu.make_async_copy(src.at[r], held.at[r], in_sem.at[i]) for i, r in enumerate(rows)]
    out = [pltpu.make_async_copy(held.at[r], dst.at[r], out_sem.at[i]) for i, r in enumerate(rows)]
    for c in into:
        c.start()
    for a, b in zip(into, out):
        a.wait()
        b.start()
    for c in out:
        c.wait()


def split(d):
    tiles = d // 128
    low = tiles // 3
    sizes = [low, low, low]
    for i in range(tiles - 3 * low):
        sizes[2 - i] += 1
    return [128 * n for n in sizes]


def solution(mesh):
    names = ("dp", "ep")

    def step(x, expert, slot, gate, w_gate, w_up, w_down, s_gate, s_up, s_down):
        R = round(mesh.shape["ep"] ** (1 / 3))
        T, D = x.shape[2:]
        top, members = expert.shape[-1], mesh.shape["ep"]
        FF, SFF = w_gate.shape[-1], s_gate.shape[-1]
        slots = 5 * T * top // (4 * members)
        parts = split(D)
        x, (expert, slot, gate) = x[0, 0], (v[0].transpose(2, 0, 1) for v in (expert, slot, gate))
        any_space = pl.BlockSpec(memory_space=pl.ANY)
        tile = min(256, SFF)
        dma = pltpu.SemaphoreType.DMA
        scratch = (
            [pltpu.VMEM((R, T, c), BF16) for c in parts]
            + [pltpu.VMEM((HALVES, R, R, R, S, c), BF16) for c in parts]
            + [pltpu.VMEM((HALVES, R - 1, R, R, S, c), BF16) for c in parts]
            + [pltpu.VMEM((HALVES, R, R, R, S, c), BF16) for c in parts]
            + [pltpu.VMEM((2, T // 2, c), F32) for c in parts]
            + [pltpu.VMEM((T, D), BF16), pltpu.VMEM((T, D), BF16), pltpu.VMEM((top, 1, T), jnp.int32), pltpu.VMEM((top, 1, T), jnp.int32),
               pltpu.VMEM((top, 1, T), F32)]
            + [pltpu.VMEM((16, T), F32), pltpu.VMEM((3, R, 16, T), F32)]
            + [pltpu.VMEM((D, FF), BF16), pltpu.VMEM((D, FF), BF16), pltpu.VMEM((FF, D), BF16)]
            + [pltpu.VMEM((R * R * S, D), BF16), pltpu.VMEM((R * R * S, FF), BF16), pltpu.VMEM((T, D), F32)]
            + [pltpu.VMEM((2, D, tile), BF16), pltpu.VMEM((2, D, tile), BF16), pltpu.VMEM((2, tile, D), BF16)]
            + [dma((3,)), dma((4,)), dma((3,)), dma((2, 3))]
            + [dma((3,))] * 3 + [dma((3, R, 2))]
            + [dma((3, HALVES)), dma((3, HALVES, R)), dma((3, HALVES)), dma((3, HALVES))]
            + [dma((3, HALVES)), dma((3, HALVES, R)), dma((3, HALVES)), dma((3, HALVES))] + [dma((3,))] * 2 + [dma((3, 2))]
            + [pltpu.SemaphoreType.REGULAR((3, HALVES))] * 2
        )
        y = pl.pallas_call(
            functools.partial(kernel, R, parts, tile, top, slots, names),
            out_shape=jax.ShapeDtypeStruct((T, D), BF16),
            in_specs=[any_space] * 10,
            out_specs=any_space,
            scratch_shapes=scratch,
            compiler_params=pltpu.CompilerParams(
                collective_id=0, has_side_effects=True, vmem_limit_bytes=67043328
            ),
            name="moe",
        )(x, expert, slot, gate, w_gate[0], w_up[0], w_down[0], s_gate, s_up, s_down)
        pieces = 8
        y = pl.pallas_call(
            functools.partial(hand_on, pieces),
            out_shape=jax.ShapeDtypeStruct((T, D), BF16),
            in_specs=[any_space],
            out_specs=any_space,
            scratch_shapes=[pltpu.VMEM((T, D), BF16), dma((pieces,)), dma((pieces,))],
            name="hand_on",
        )(y)
        return y[None, None]

    tok = P("dp", "ep", None, None)
    exp = P("ep", None, None)
    rep = P(None, None)
    return jax.shard_map(
        step, mesh=mesh,
        in_specs=(tok, tok, tok, tok, exp, exp, exp, rep, rep, rep),
        out_specs=tok, check_vma=False,
    )
```

```python
import functools

import jax
import jax.numpy as jnp
from jax import lax
from jax.experimental import pallas as pl
from jax.experimental.pallas import tpu as pltpu
from jax.sharding import PartitionSpec as P

MESH = pl.DeviceIdType.MESH
BF16, F32 = jnp.bfloat16, jnp.float32
S = 16
HALVES = 2
SPAN = S * HALVES
ALL = slice(None)


def silu_mul(g, u):
    return (jax.nn.silu(g) * u).astype(BF16)


def kernel(R, parts, shared_tile, top, slots, names, *refs):
    (x_hbm, e_hbm, s_hbm, gate_hbm, wg_hbm, wu_hbm, wd_hbm, sg_hbm, su_hbm, sd_hbm, y_hbm) = refs[:11]
    xa, g_buf, h_buf, z_buf, own = (refs[i:i + 3] for i in range(11, 26, 3))
    (y_ref, x_ref, e_ref, s_ref, gate_ref, m_ref, meta, wg, wu, wd, zcat, hb, yacc, sgb, sub, sdb,
     out_sem, in_sem, w_sem, sh_sem, m_s, m_r, a_s, a_r, b_s, b_r, c_s, c_r, c2_s, c2_r, b2_s, b2_r, a2_s, a2_r, ah_r, h_free, g_free) = refs[26:]
    dp_axis, ep_axis = names
    T = x_ref.shape[0]
    FF = wg.shape[1]
    KR = R * R * S
    dp, me = lax.axis_index(dp_axis), lax.axis_index(ep_axis)
    pos = (me // (R * R), lax.rem(me // R, R), lax.rem(me, R))
    unit = (R * R, R, 1)
    edges = [0]
    for c in parts:
        edges.append(edges[-1] + c)
    cols = [slice(edges[k], edges[k + 1]) for k in range(3)]

    order = sorted(range(3), key=lambda k: -parts[k])
    near = sorted(range(1, R), key=lambda r: (min(r, R - r), -r))
    ring4 = R == 4
    back = (0, 2, 1)
    lo, hi = pl.ds(0, T // 2), pl.ds(T // 2, T // 2)

    def peer(axis, r):
        return me + (lax.rem(pos[axis] + r, R) - pos[axis]) * unit[axis]

    def zsl(k, a, b, c):
        i = [None] * 3
        i[k], i[(k + 1) % 3], i[(k + 2) % 3] = a, b, c
        return tuple(i)

    def hsl(k, a, b):
        return (a, b) if k < 2 else (b, a)

    def send(src, dst, s, r, axis, step):
        pltpu.make_async_remote_copy(
            src_ref=src, dst_ref=dst, send_sem=s, recv_sem=r,
            device_id=(dp, peer(axis, step)), device_id_type=MESH,
        ).start()

    def pend(ref, s, r):
        return pltpu.make_async_remote_copy(
            src_ref=ref, dst_ref=ref, send_sem=s, recv_sem=r,
            device_id=(dp, peer(0, 1)), device_id_type=MESH,
        )

    def whole(k, h):
        return g_buf[k].at[h, 1:R]

    n_sh = sg_hbm.shape[1] // shared_tile

    def sh_copies(j, slot):
        at = pl.ds(pl.multiple_of(j * shared_tile, shared_tile), shared_tile)
        return (
            pltpu.make_async_copy(sg_hbm.at[:, at], sgb.at[slot], sh_sem.at[slot, 0]),
            pltpu.make_async_copy(su_hbm.at[:, at], sub.at[slot], sh_sem.at[slot, 1]),
            pltpu.make_async_copy(sd_hbm.at[at], sdb.at[slot], sh_sem.at[slot, 2]),
        )

    in_copies = [
        pltpu.make_async_copy(src, dst, in_sem.at[i])
        for i, (src, dst) in enumerate(((x_hbm, x_ref), (e_hbm, e_ref), (s_hbm, s_ref), (gate_hbm, gate_ref)))
    ]
    for c in in_copies:
        c.start()

    def shared(j):
        slot = lax.rem(j, 2)
        for c in sh_copies(j, slot):
            c.wait()

        @pl.when(j + 1 < n_sh)
        def _():
            for c in sh_copies(j + 1, 1 - slot):
                c.start()

        g = jnp.dot(x_ref[...], sgb[slot], preferred_element_type=F32)
        u = jnp.dot(x_ref[...], sub[slot], preferred_element_type=F32)
        yacc[...] += jnp.dot(silu_mul(g, u), sdb[slot], preferred_element_type=F32)

    def slot_ids(k, h):
        row = lax.broadcasted_iota(jnp.int32, (KR, T), 0)
        rb, rc, s = row // (R * S), lax.rem(row // S, R), lax.rem(row, S)
        b, c = (k + 1) % 3, (k + 2) % 3
        e = pos[k] * unit[k] + lax.rem(rb + pos[b], R) * unit[b] + lax.rem(rc + pos[c], R) * unit[c]
        return (e * SPAN + s + h * S).astype(F32)

    def gather(k, h, ra, ids):
        hit = ids == meta[k, ra, 0:1, :]
        for j in range(1, top):
            hit = hit | (ids == meta[k, ra, j:j + 1, :])
        pick = jnp.where(hit, 1.0, 0.0).astype(BF16)
        rows = jnp.dot(pick, xa[k][ra], preferred_element_type=F32).astype(BF16)
        rows = rows.reshape(R, R, S, parts[k])
        g_buf[k][h, 1:R, :, ra] = rows[1:]
        z_buf[k][(h,) + zsl(k, ra, 0, 0)] = rows[0, 0]
        h_buf[k][(h, ALL) + hsl(k, ra, 0)] = rows[0, 1:]

    def send_b(k, h, ra):
        for rb in near:
            to = R - rb
            send(g_buf[k].at[h, rb, 1:R, ra], h_buf[k].at[(h, ALL) + hsl(k, ra, to)],
                 b_s.at[k, h], b_r.at[k, h, ra], (k + 1) % 3, rb)
            send(g_buf[k].at[h, rb, 0, ra], z_buf[k].at[(h,) + zsl(k, ra, to, 0)],
                 b_s.at[k, h], b_r.at[k, h, ra], (k + 1) % 3, rb)

    @jax.named_scope("relay_c")
    def relay_c(h, ra):
        for k in order:
            pend(g_buf[k].at[h, 1:R, :, 0], b_s.at[k, h], b_r.at[k, h, ra]).wait_recv()
            for rc in near:
                send(h_buf[k].at[(h, rc - 1) + hsl(k, ra, ALL)], z_buf[k].at[(h,) + zsl(k, ra, ALL, R - rc)],
                     c_s.at[k, h], c_r.at[k, h], (k + 2) % 3, rc)

    barrier = pltpu.get_barrier_semaphore()
    for axis in range(3):
        for r in range(1, R):
            pl.semaphore_signal(barrier, inc=1, device_id=(dp, peer(axis, r)), device_id_type=MESH)

    for c in sh_copies(0, 0):
        c.start()
    for c in in_copies[1:]:
        c.wait()
    m_ref[...] = jnp.zeros_like(m_ref)
    for j in range(top):
        m_ref[j:j + 1, :] = jnp.where(s_ref[j] < slots, e_ref[j] * SPAN + s_ref[j], -1).astype(F32)
        m_ref[8 + j:9 + j, :] = gate_ref[j].astype(BF16).astype(F32)
    in_copies[0].wait()
    with jax.named_scope("barrier"):
        pl.semaphore_wait(barrier, 3 * (R - 1))

    for k in order:
        for r in near:
            send(m_ref, meta.at[k, R - r], m_s.at[k], m_r.at[k], k, r)
    halves = {1: (lo, hi), 3: (hi, lo)} if ring4 else {r: (lo, hi) for r in near}
    for i in range(2):
        for r in halves:
            at = halves[r][i]
            for k in order:
                send(x_ref.at[at, cols[k]], xa[k].at[R - r, at], a_s.at[k], a_r.at[k, R - r, i], k, r)
    for k in range(3):
        meta[k, 0] = m_ref[...]
        xa[k][0] = x_ref[:, cols[k]]
    yacc[...] = jnp.zeros_like(yacc)
    for k in order:
        gather(k, 0, 0, slot_ids(k, 0))

    late = 2 * R - 1
    early = max(n_sh - late, 0)

    @jax.named_scope("wait_a")
    def wait_a(k, ra, i):
        pend(xa[k].at[ra, lo], a_s.at[k], a_r.at[k, ra, i]).wait_recv()

    @jax.named_scope("gather")
    def gather_all(h, ra, go):
        for k in order:
            gather(k, h, ra, slot_ids(k, h))
            if go:
                send_b(k, h, ra)

    pl.loop(0, early // 2)(jax.named_scope("shared")(shared))
    if ring4:
        seq = [0, 3, 1, 2]
        for k in order:
            wait_a(k, 3, 0)
            send(xa[k].at[3, lo], xa[k].at[2, lo], a_s.at[k], a_r.at[k, 2, 0], k, 1)
            wait_a(k, 1, 0)
            send(xa[k].at[1, hi], xa[k].at[2, hi], a_s.at[k], a_r.at[k, 2, 1], k, 3)
    else:
        seq = list(range(R))
        for r in near:
            for k in order:
                wait_a(k, r, 0)
    for k in order:
        send_b(k, 0, 0)
    pl.loop(early // 2, early)(jax.named_scope("shared")(shared))
    for k in order:
        with jax.named_scope("wait_m"):
            pend(meta.at[k, 1:R], m_s.at[k], m_r.at[k]).wait_recv()
    for ra in seq[1:]:
        for k in order:
            if ring4 and ra == 2:
                wait_a(k, ra, 0)
            wait_a(k, ra, 1)
        gather_all(0, ra, True)

    w_copies = [
        pltpu.make_async_copy(src, dst, w_sem.at[i])
        for i, (src, dst) in enumerate(((wg_hbm, wg), (wu_hbm, wu), (wd_hbm, wd)))
    ]
    for c in w_copies:
        c.start()

    @pl.loop(0, R)
    def _(ra):
        gather_all(1, ra, False)

    @pl.loop(0, late)
    def _(i):
        for step, ra in enumerate(seq):
            @pl.when(i == 2 * step)
            def _():
                relay_c(0, ra)
                for k in order:
                    send_b(k, 1, ra)

        @pl.when(early + i < n_sh)
        @jax.named_scope("shared")
        def _():
            shared(early + i)

    for c in w_copies:
        c.wait()
    for ra in seq[:-1]:
        relay_c(1, ra)

    def send_c2(h, rx):
        for k in order:
            s, axis = c2_s.at[k, h], (back[k] + 2) % 3
            z, hh, g = z_buf[k], h_buf[k], g_buf[k]
            if back[k] == 0:
                for rc in near:
                    send(z.at[h, rx, 1:R, rc], hh.at[h, R - rc - 1, rx, 1:R], s, c2_r.at[k, h, R - rc], axis, rc)
                    send(z.at[h, rx, 0, rc], g.at[h, 0, R - rc, rx], s, c2_r.at[k, h, R - rc], axis, rc)
            elif back[k] == 1:
                @pl.when(rx > 0)
                def _():
                    send(z.at[h, rx, :, 1:R], hh.at[h, R - rx - 1, :, 1:R], s, c2_r.at[k, h, R - rx], axis, rx)
                    send(z.at[h, rx, :, 0], g.at[h, 0, R - rx], s, c2_r.at[k, h, R - rx], axis, rx)
            else:
                @pl.when(rx > 0)
                def _():
                    for rc in near:
                        send(z.at[h, rx, rc], hh.at[h, R - rc - 1, rx], s, c2_r.at[k, h, R - rc], axis, rc)

                @pl.when(rx == 0)
                def _():
                    for rc in near:
                        send(z.at[h, rx, rc], g.at[h, 0, R - rc], s, c2_r.at[k, h, R - rc], axis, rc)

    def own_b2(h):
        for k in order:
            pl.semaphore_wait(g_free.at[k, h], R - 1)
            for rb in near:
                send(z_buf[k].at[(h,) + zsl(back[k], ALL, rb, 0)], g_buf[k].at[h, R - rb, 0],
                     b2_s.at[k, h], b2_r.at[k, h], (back[k] + 1) % 3, rb)

    @jax.named_scope("relay_b2")
    def relay_b2(h):
        for ce in range(1, R):
            for k in order:
                pend(g_buf[k].at[h, 1], c2_s.at[k, h], c2_r.at[k, h, ce]).wait_recv()
                for rb in near:
                    send(h_buf[k].at[(h, ce - 1) + hsl(back[k], ALL, rb)], g_buf[k].at[h, R - rb, ce],
                         b2_s.at[k, h], b2_r.at[k, h], (back[k] + 1) % 3, rb)

    wide = [(n, min(512, FF - n)) for n in range(0, FF, 512)]

    @pl.loop(0, HALVES * R)
    def _(t):
        h, i = t // R, lax.rem(t, R)
        rx = R - 1 - i

        @pl.when(i == 0)
        @jax.named_scope("wait_c")
        def _():
            for k in range(3):
                pend(whole(k, h), c_s.at[k, h], c_r.at[k, h]).wait_recv()
            @pl.when(t == 0)
            def _():
                for k in range(3):
                    pend(xa[k].at[1:R], a_s.at[k], a2_r.at[k]).wait_send()

            for k in range(3):
                pend(whole(k, h), c_s.at[k, h], c_r.at[k, h]).wait_send()
                pend(whole(k, h), b_s.at[k, h], b_r.at[k, h]).wait_send()
                for free, axis in ((h_free, back[k] + 2), (g_free, back[k] + 1)):
                    for r in range(1, R):
                        pl.semaphore_signal(free.at[k, h], inc=1, device_id=(dp, peer(axis % 3, r)), device_id_type=MESH)

        with jax.named_scope("up"):
            for k in range(3):
                zcat[:, cols[k]] = z_buf[k][h, rx].reshape(KR, parts[k])
            for n, w in wide:
                g = jnp.dot(zcat[...], wg[:, n:n + w], preferred_element_type=F32)
                u = jnp.dot(zcat[...], wu[:, n:n + w], preferred_element_type=F32)
                hb[:, n:n + w] = silu_mul(g, u)
        with jax.named_scope("down"):
            for k in range(3):
                o = jnp.dot(hb[...], wd[:, cols[k]], preferred_element_type=F32)
                z_buf[k][h, rx] = o.astype(BF16).reshape(R, R, S, parts[k])

        @pl.when(i == 0)
        def _():
            for k in range(3):
                pl.semaphore_wait(h_free.at[k, h], R - 1)

        send_c2(h, rx)

        @pl.when(t == 0)
        def _():
            relay_c(1, seq[-1])

        @pl.when(i == R - 1)
        def _():
            own_b2(h)

        @pl.when(t == R)
        def _():
            relay_b2(0)

    def own_rows(k, h):
        g_buf[k][h, 0, 0] = z_buf[k][(h,) + zsl(back[k], ALL, 0, 0)]

    wide_w = HALVES * KR
    across = FF // wide_w

    def block(k, ra):
        i = k * R + ra
        return pl.ds(i // across * T, T), pl.ds(i % across * wide_w, wide_w)

    @jax.named_scope("weights")
    def build(k, ra):
        rows, columns = block(k, ra)
        for h in range(HALVES):
            ids = slot_ids(back[k], h)
            w = jnp.zeros((KR, T), F32)
            for j in range(top):
                w += jnp.where(ids == meta[back[k], ra, j:j + 1, :], meta[back[k], ra, 8 + j:9 + j, :], 0.0)
            wg[rows, pl.ds(columns.start + h * KR, KR)] = w.T.astype(BF16)

    def partial(k, ra):
        rows = g_buf[k][:, :, :, ra].reshape(wide_w, parts[k])
        return jnp.dot(wg[block(k, ra)], rows, preferred_element_type=F32)

    relay_b2(1)
    for k in order:
        for h in range(HALVES):
            own_rows(k, h)
    for ra in [2, 1, 3, 0] if ring4 else range(R):
        for k in order:
            build(k, ra)
    for k in order:
        with jax.named_scope("wait_b2"):
            pend(whole(k, 0), b2_s.at[k, 0], b2_r.at[k, 0]).wait_recv()
    for k in order:
        with jax.named_scope("wait_b2"):
            pend(whole(k, 1), b2_s.at[k, 1], b2_r.at[k, 1]).wait_recv()

    def ps(k, ra, at):
        beside = k == 2 and parts[0] + parts[2] <= FF
        row = ((0 if beside else k) * (R - 1) + ra - 1) * T + at.start
        left = parts[0] if beside else 0
        return wu.at[pl.ds(row, at.size), pl.ds(left, parts[k])]

    def send_a2(k, ra, at):
        send(ps(k, ra, at), xa[k].at[R - ra, at], a2_s.at[k], a2_r.at[k], back[k], ra)

    if ring4:
        for k in order:
            with jax.named_scope("weigh_far"):
                ps(k, 2, pl.ds(0, T))[...] = partial(k, 2).astype(BF16)
            send(ps(k, 2, lo), xa[k].at[2, lo], a2_s.at[k], ah_r.at[k, 0], back[k], 1)
            send(ps(k, 2, hi), xa[k].at[2, hi], a2_s.at[k], ah_r.at[k, 1], back[k], 3)
        for k in order:
            with jax.named_scope("weigh_near"):
                for i, (ra, now, later) in enumerate(((1, hi, lo), (3, lo, hi))):
                    p = partial(k, ra)
                    ps(k, ra, now)[...] = p[now.start:now.start + now.size].astype(BF16)
                    send_a2(k, ra, now)
                    own[k][i] = p[later.start:later.start + later.size]
        for k in order:
            for i, (ra, at) in enumerate(((1, lo), (3, hi))):
                with jax.named_scope("weigh_sum"):
                    pend(xa[k].at[2, at], a2_s.at[k], ah_r.at[k, i]).wait_recv()
                    ps(k, ra, at)[...] = (own[k][i] + xa[k][2, at].astype(F32)).astype(BF16)
                    send_a2(k, ra, at)
    else:
        for k in order:
            for ra in range(1, R):
                ps(k, ra, pl.ds(0, T))[...] = partial(k, ra).astype(BF16)
                send_a2(k, ra, pl.ds(0, T))
    senders = (1, 3) if ring4 else tuple(range(1, R))

    for k in order:
        with jax.named_scope("weigh_own"):
            yacc[:, cols[k]] += partial(k, 0)
    for k in order:
        with jax.named_scope("wait_a2"):
            pend(xa[k].at[0:len(senders)], a2_s.at[k], a2_r.at[k]).wait_recv()
        total = yacc[:, cols[k]]
        for ra in senders:
            total += xa[k][ra].astype(F32)
        y_ref[:, cols[k]] = total.astype(BF16)
        pltpu.make_async_copy(y_ref.at[:, cols[k]], y_hbm.at[:, cols[k]], out_sem.at[k]).start()

    for k in range(3):
        pltpu.make_async_copy(y_ref.at[:, cols[k]], y_hbm.at[:, cols[k]], out_sem.at[k]).wait()
        pend(meta.at[k, 1:R], m_s.at[k], m_r.at[k]).wait_send()
        pend(xa[k].at[1:R], a2_s.at[k], a2_r.at[k]).wait_send()
        for h in range(HALVES):
            for s, r in ((c2_s, c2_r), (b2_s, b2_r)):
                pend(whole(k, h), s.at[k, h], r.at[k, h]).wait_send()


def hand_on(pieces, src, dst, held, in_sem, out_sem):
    n = src.shape[0] // pieces
    rows = [pl.ds(i * n, n) for i in range(pieces)]
    into = [pltpu.make_async_copy(src.at[r], held.at[r], in_sem.at[i]) for i, r in enumerate(rows)]
    out = [pltpu.make_async_copy(held.at[r], dst.at[r], out_sem.at[i]) for i, r in enumerate(rows)]
    for c in into:
        c.start()
    for a, b in zip(into, out):
        a.wait()
        b.start()
    for c in out:
        c.wait()


def split(d):
    tiles = d // 128
    low = tiles // 3
    sizes = [low, low, low]
    for i in range(tiles - 3 * low):
        sizes[2 - i] += 1
    return [128 * n for n in sizes]


def solution(mesh):
    names = ("dp", "ep")

    def step(x, expert, slot, gate, w_gate, w_up, w_down, s_gate, s_up, s_down):
        R = round(mesh.shape["ep"] ** (1 / 3))
        T, D = x.shape[2:]
        top, members = expert.shape[-1], mesh.shape["ep"]
        FF, SFF = w_gate.shape[-1], s_gate.shape[-1]
        slots = 5 * T * top // (4 * members)
        parts = split(D)
        x, (expert, slot, gate) = x[0, 0], (v[0].transpose(2, 0, 1) for v in (expert, slot, gate))
        any_space = pl.BlockSpec(memory_space=pl.ANY)
        tile = min(256, SFF)
        dma = pltpu.SemaphoreType.DMA
        scratch = (
            [pltpu.VMEM((R, T, c), BF16) for c in parts]
            + [pltpu.VMEM((HALVES, R, R, R, S, c), BF16) for c in parts]
            + [pltpu.VMEM((HALVES, R - 1, R, R, S, c), BF16) for c in parts]
            + [pltpu.VMEM((HALVES, R, R, R, S, c), BF16) for c in parts]
            + [pltpu.VMEM((2, T // 2, c), F32) for c in parts]
            + [pltpu.VMEM((T, D), BF16), pltpu.VMEM((T, D), BF16), pltpu.VMEM((top, 1, T), jnp.int32), pltpu.VMEM((top, 1, T), jnp.int32),
               pltpu.VMEM((top, 1, T), F32)]
            + [pltpu.VMEM((16, T), F32), pltpu.VMEM((3, R, 16, T), F32)]
            + [pltpu.VMEM((D, FF), BF16), pltpu.VMEM((D, FF), BF16), pltpu.VMEM((FF, D), BF16)]
            + [pltpu.VMEM((R * R * S, D), BF16), pltpu.VMEM((R * R * S, FF), BF16), pltpu.VMEM((T, D), F32)]
            + [pltpu.VMEM((2, D, tile), BF16), pltpu.VMEM((2, D, tile), BF16), pltpu.VMEM((2, tile, D), BF16)]
            + [dma((3,)), dma((4,)), dma((3,)), dma((2, 3))]
            + [dma((3,))] * 3 + [dma((3, R, 2))]
            + [dma((3, HALVES)), dma((3, HALVES, R)), dma((3, HALVES)), dma((3, HALVES))]
            + [dma((3, HALVES)), dma((3, HALVES, R)), dma((3, HALVES)), dma((3, HALVES))] + [dma((3,))] * 2 + [dma((3, 2))]
            + [pltpu.SemaphoreType.REGULAR((3, HALVES))] * 2
        )
        y = pl.pallas_call(
            functools.partial(kernel, R, parts, tile, top, slots, names),
            out_shape=jax.ShapeDtypeStruct((T, D), BF16),
            in_specs=[any_space] * 10,
            out_specs=any_space,
            scratch_shapes=scratch,
            compiler_params=pltpu.CompilerParams(
                collective_id=0, has_side_effects=True, vmem_limit_bytes=67043328
            ),
            name="moe",
        )(x, expert, slot, gate, w_gate[0], w_up[0], w_down[0], s_gate, s_up, s_down)
        pieces = 8
        y = pl.pallas_call(
            functools.partial(hand_on, pieces),
            out_shape=jax.ShapeDtypeStruct((T, D), BF16),
            in_specs=[any_space],
            out_specs=any_space,
            scratch_shapes=[pltpu.VMEM((T, D), BF16), dma((pieces,)), dma((pieces,))],
            name="hand_on",
        )(y)
        return y[None, None]

    tok = P("dp", "ep", None, None)
    exp = P("ep", None, None)
    rep = P(None, None)
    return jax.shard_map(
        step, mesh=mesh,
        in_specs=(tok, tok, tok, tok, exp, exp, exp, rep, rep, rep),
        out_specs=tok, check_vma=False,
    )
```

```python
import functools

import jax
import jax.numpy as jnp
from jax import lax
from jax.experimental import pallas as pl
from jax.experimental.pallas import tpu as pltpu
from jax.sharding import PartitionSpec as P

MESH = pl.DeviceIdType.MESH
BF16, F32 = jnp.bfloat16, jnp.float32
S = 16
HALVES = 2
SPAN = S * HALVES
ALL = slice(None)


def silu_mul(g, u):
    return (jax.nn.silu(g) * u).astype(BF16)


def kernel(R, parts, shared_tile, top, slots, names, *refs):
    (x_hbm, e_hbm, s_hbm, gate_hbm, wg_hbm, wu_hbm, wd_hbm, sg_hbm, su_hbm, sd_hbm, y_hbm) = refs[:11]
    xa, g_buf, h_buf, z_buf, own = (refs[i:i + 3] for i in range(11, 26, 3))
    (y_ref, x_ref, e_ref, s_ref, gate_ref, m_ref, meta, wg, wu, wd, zcat, hb, yacc, sgb, sub, sdb,
     out_sem, in_sem, w_sem, sh_sem, m_s, m_r, a_s, a_r, b_s, b_r, c_s, c_r, c2_s, c2_r, b2_s, b2_r, a2_s, a2_r, ah_r, h_free, g_free) = refs[26:]
    dp_axis, ep_axis = names
    T = x_ref.shape[0]
    FF = wg.shape[1]
    KR = R * R * S
    dp, me = lax.axis_index(dp_axis), lax.axis_index(ep_axis)
    pos = (me // (R * R), lax.rem(me // R, R), lax.rem(me, R))
    unit = (R * R, R, 1)
    edges = [0]
    for c in parts:
        edges.append(edges[-1] + c)
    cols = [slice(edges[k], edges[k + 1]) for k in range(3)]

    order = sorted(range(3), key=lambda k: -parts[k])
    near = sorted(range(1, R), key=lambda r: (min(r, R - r), -r))
    ring4 = R == 4
    back = (0, 1, 2)
    lo, hi = pl.ds(0, T // 2), pl.ds(T // 2, T // 2)

    def peer(axis, r):
        return me + (lax.rem(pos[axis] + r, R) - pos[axis]) * unit[axis]

    def zsl(k, a, b, c):
        i = [None] * 3
        i[k], i[(k + 1) % 3], i[(k + 2) % 3] = a, b, c
        return tuple(i)

    def hsl(k, a, b):
        return (a, b) if k < 2 else (b, a)

    def send(src, dst, s, r, axis, step):
        pltpu.make_async_remote_copy(
            src_ref=src, dst_ref=dst, send_sem=s, recv_sem=r,
            device_id=(dp, peer(axis, step)), device_id_type=MESH,
        ).start()

    def pend(ref, s, r):
        return pltpu.make_async_remote_copy(
            src_ref=ref, dst_ref=ref, send_sem=s, recv_sem=r,
            device_id=(dp, peer(0, 1)), device_id_type=MESH,
        )

    def whole(k, h):
        return g_buf[k].at[h, 1:R]

    n_sh = sg_hbm.shape[1] // shared_tile

    def sh_copies(j, slot):
        at = pl.ds(pl.multiple_of(j * shared_tile, shared_tile), shared_tile)
        return (
            pltpu.make_async_copy(sg_hbm.at[:, at], sgb.at[slot], sh_sem.at[slot, 0]),
            pltpu.make_async_copy(su_hbm.at[:, at], sub.at[slot], sh_sem.at[slot, 1]),
            pltpu.make_async_copy(sd_hbm.at[at], sdb.at[slot], sh_sem.at[slot, 2]),
        )

    in_copies = [
        pltpu.make_async_copy(src, dst, in_sem.at[i])
        for i, (src, dst) in enumerate(((x_hbm, x_ref), (e_hbm, e_ref), (s_hbm, s_ref), (gate_hbm, gate_ref)))
    ]
    for c in in_copies:
        c.start()

    def shared(j):
        slot = lax.rem(j, 2)
        for c in sh_copies(j, slot):
            c.wait()

        @pl.when(j + 1 < n_sh)
        def _():
            for c in sh_copies(j + 1, 1 - slot):
                c.start()

        g = jnp.dot(x_ref[...], sgb[slot], preferred_element_type=F32)
        u = jnp.dot(x_ref[...], sub[slot], preferred_element_type=F32)
        yacc[...] += jnp.dot(silu_mul(g, u), sdb[slot], preferred_element_type=F32)

    def slot_ids(k, h):
        row = lax.broadcasted_iota(jnp.int32, (KR, T), 0)
        rb, rc, s = row // (R * S), lax.rem(row // S, R), lax.rem(row, S)
        b, c = (k + 1) % 3, (k + 2) % 3
        e = pos[k] * unit[k] + lax.rem(rb + pos[b], R) * unit[b] + lax.rem(rc + pos[c], R) * unit[c]
        return (e * SPAN + s + h * S).astype(F32)

    def gather(k, h, ra, ids):
        hit = ids == meta[k, ra, 0:1, :]
        for j in range(1, top):
            hit = hit | (ids == meta[k, ra, j:j + 1, :])
        pick = jnp.where(hit, 1.0, 0.0).astype(BF16)
        rows = jnp.dot(pick, xa[k][ra], preferred_element_type=F32).astype(BF16)
        rows = rows.reshape(R, R, S, parts[k])
        g_buf[k][h, 1:R, :, ra] = rows[1:]
        z_buf[k][(h,) + zsl(k, ra, 0, 0)] = rows[0, 0]
        h_buf[k][(h, ALL) + hsl(k, ra, 0)] = rows[0, 1:]

    def send_b(k, h, ra):
        for rb in near:
            to = R - rb
            send(g_buf[k].at[h, rb, 1:R, ra], h_buf[k].at[(h, ALL) + hsl(k, ra, to)],
                 b_s.at[k, h], b_r.at[k, h, ra], (k + 1) % 3, rb)
            send(g_buf[k].at[h, rb, 0, ra], z_buf[k].at[(h,) + zsl(k, ra, to, 0)],
                 b_s.at[k, h], b_r.at[k, h, ra], (k + 1) % 3, rb)

    @jax.named_scope("relay_c")
    def relay_c(h, ra):
        for k in order:
            pend(g_buf[k].at[h, 1:R, :, 0], b_s.at[k, h], b_r.at[k, h, ra]).wait_recv()
            for rc in near:
                send(h_buf[k].at[(h, rc - 1) + hsl(k, ra, ALL)], z_buf[k].at[(h,) + zsl(k, ra, ALL, R - rc)],
                     c_s.at[k, h], c_r.at[k, h], (k + 2) % 3, rc)

    barrier = pltpu.get_barrier_semaphore()
    for axis in range(3):
        for r in range(1, R):
            pl.semaphore_signal(barrier, inc=1, device_id=(dp, peer(axis, r)), device_id_type=MESH)

    for c in sh_copies(0, 0):
        c.start()
    for c in in_copies[1:]:
        c.wait()
    m_ref[...] = jnp.zeros_like(m_ref)
    for j in range(top):
        m_ref[j:j + 1, :] = jnp.where(s_ref[j] < slots, e_ref[j] * SPAN + s_ref[j], -1).astype(F32)
        m_ref[8 + j:9 + j, :] = gate_ref[j].astype(BF16).astype(F32)
    in_copies[0].wait()
    with jax.named_scope("barrier"):
        pl.semaphore_wait(barrier, 3 * (R - 1))

    for k in order:
        for r in near:
            send(m_ref, meta.at[k, R - r], m_s.at[k], m_r.at[k], k, r)
    halves = {1: (lo, hi), 3: (hi, lo)} if ring4 else {r: (lo, hi) for r in near}
    for i in range(2):
        for r in halves:
            at = halves[r][i]
            for k in order:
                send(x_ref.at[at, cols[k]], xa[k].at[R - r, at], a_s.at[k], a_r.at[k, R - r, i], k, r)
    for k in range(3):
        meta[k, 0] = m_ref[...]
        xa[k][0] = x_ref[:, cols[k]]
    yacc[...] = jnp.zeros_like(yacc)
    for k in order:
        gather(k, 0, 0, slot_ids(k, 0))

    late = 2 * R - 1
    early = max(n_sh - late, 0)

    @jax.named_scope("wait_a")
    def wait_a(k, ra, i):
        pend(xa[k].at[ra, lo], a_s.at[k], a_r.at[k, ra, i]).wait_recv()

    @jax.named_scope("gather")
    def gather_all(h, ra, go):
        for k in order:
            gather(k, h, ra, slot_ids(k, h))
            if go:
                send_b(k, h, ra)

    pl.loop(0, early // 2)(jax.named_scope("shared")(shared))
    if ring4:
        seq = [0, 3, 1, 2]
        for k in order:
            wait_a(k, 3, 0)
            send(xa[k].at[3, lo], xa[k].at[2, lo], a_s.at[k], a_r.at[k, 2, 0], k, 1)
            wait_a(k, 1, 0)
            send(xa[k].at[1, hi], xa[k].at[2, hi], a_s.at[k], a_r.at[k, 2, 1], k, 3)
    else:
        seq = list(range(R))
        for r in near:
            for k in order:
                wait_a(k, r, 0)
    for k in order:
        send_b(k, 0, 0)
    pl.loop(early // 2, early)(jax.named_scope("shared")(shared))
    for k in order:
        with jax.named_scope("wait_m"):
            pend(meta.at[k, 1:R], m_s.at[k], m_r.at[k]).wait_recv()
    for ra in seq[1:]:
        for k in order:
            if ring4 and ra == 2:
                wait_a(k, ra, 0)
            wait_a(k, ra, 1)
        gather_all(0, ra, True)

    w_copies = [
        pltpu.make_async_copy(src, dst, w_sem.at[i])
        for i, (src, dst) in enumerate(((wg_hbm, wg), (wu_hbm, wu), (wd_hbm, wd)))
    ]
    for c in w_copies:
        c.start()

    @pl.loop(0, R)
    def _(ra):
        gather_all(1, ra, False)

    @pl.loop(0, late)
    def _(i):
        for step, ra in enumerate(seq):
            @pl.when(i == 2 * step)
            def _():
                relay_c(0, ra)
                for k in order:
                    send_b(k, 1, ra)

        @pl.when(early + i < n_sh)
        @jax.named_scope("shared")
        def _():
            shared(early + i)

    for c in w_copies:
        c.wait()
    for ra in seq[:-1]:
        relay_c(1, ra)

    def send_c2(h, rx):
        for k in order:
            s, axis = c2_s.at[k, h], (back[k] + 2) % 3
            z, hh, g = z_buf[k], h_buf[k], g_buf[k]
            if back[k] == 0:
                for rc in near:
                    send(z.at[h, rx, 1:R, rc], hh.at[h, R - rc - 1, rx, 1:R], s, c2_r.at[k, h, R - rc], axis, rc)
                    send(z.at[h, rx, 0, rc], g.at[h, 0, R - rc, rx], s, c2_r.at[k, h, R - rc], axis, rc)
            elif back[k] == 1:
                @pl.when(rx > 0)
                def _():
                    send(z.at[h, rx, :, 1:R], hh.at[h, R - rx - 1, :, 1:R], s, c2_r.at[k, h, R - rx], axis, rx)
                    send(z.at[h, rx, :, 0], g.at[h, 0, R - rx], s, c2_r.at[k, h, R - rx], axis, rx)
            else:
                @pl.when(rx > 0)
                def _():
                    for rc in near:
                        send(z.at[h, rx, rc], hh.at[h, R - rc - 1, rx], s, c2_r.at[k, h, R - rc], axis, rc)

                @pl.when(rx == 0)
                def _():
                    for rc in near:
                        send(z.at[h, rx, rc], g.at[h, 0, R - rc], s, c2_r.at[k, h, R - rc], axis, rc)

    def own_b2(h):
        for k in order:
            pl.semaphore_wait(g_free.at[k, h], R - 1)
            for rb in near:
                send(z_buf[k].at[(h,) + zsl(back[k], ALL, rb, 0)], g_buf[k].at[h, R - rb, 0],
                     b2_s.at[k, h], b2_r.at[k, h], (back[k] + 1) % 3, rb)

    @jax.named_scope("relay_b2")
    def relay_b2(h):
        for ce in range(1, R):
            for k in order:
                pend(g_buf[k].at[h, 1], c2_s.at[k, h], c2_r.at[k, h, ce]).wait_recv()
                for rb in near:
                    send(h_buf[k].at[(h, ce - 1) + hsl(back[k], ALL, rb)], g_buf[k].at[h, R - rb, ce],
                         b2_s.at[k, h], b2_r.at[k, h], (back[k] + 1) % 3, rb)

    wide = [(n, min(512, FF - n)) for n in range(0, FF, 512)]

    @pl.loop(0, HALVES * R)
    def _(t):
        h, i = t // R, lax.rem(t, R)
        rx = R - 1 - i

        @pl.when(i == 0)
        @jax.named_scope("wait_c")
        def _():
            for k in range(3):
                pend(whole(k, h), c_s.at[k, h], c_r.at[k, h]).wait_recv()
            @pl.when(t == 0)
            def _():
                for k in range(3):
                    pend(xa[k].at[1:R], a_s.at[k], a2_r.at[k]).wait_send()

            for k in range(3):
                pend(whole(k, h), c_s.at[k, h], c_r.at[k, h]).wait_send()
                pend(whole(k, h), b_s.at[k, h], b_r.at[k, h]).wait_send()
                for free, axis in ((h_free, back[k] + 2), (g_free, back[k] + 1)):
                    for r in range(1, R):
                        pl.semaphore_signal(free.at[k, h], inc=1, device_id=(dp, peer(axis % 3, r)), device_id_type=MESH)

        with jax.named_scope("up"):
            for k in range(3):
                zcat[:, cols[k]] = z_buf[k][h, rx].reshape(KR, parts[k])
            for n, w in wide:
                g = jnp.dot(zcat[...], wg[:, n:n + w], preferred_element_type=F32)
                u = jnp.dot(zcat[...], wu[:, n:n + w], preferred_element_type=F32)
                hb[:, n:n + w] = silu_mul(g, u)
        with jax.named_scope("down"):
            for k in range(3):
                o = jnp.dot(hb[...], wd[:, cols[k]], preferred_element_type=F32)
                z_buf[k][h, rx] = o.astype(BF16).reshape(R, R, S, parts[k])

        @pl.when(i == 0)
        def _():
            for k in range(3):
                pl.semaphore_wait(h_free.at[k, h], R - 1)

        send_c2(h, rx)

        @pl.when(t == 0)
        def _():
            relay_c(1, seq[-1])

        @pl.when(i == R - 1)
        def _():
            own_b2(h)

        @pl.when(t == R)
        def _():
            relay_b2(0)

    def own_rows(k, h):
        g_buf[k][h, 0, 0] = z_buf[k][(h,) + zsl(back[k], ALL, 0, 0)]

    wide_w = HALVES * KR
    across = FF // wide_w

    def block(k, ra):
        i = k * R + ra
        return pl.ds(i // across * T, T), pl.ds(i % across * wide_w, wide_w)

    @jax.named_scope("weights")
    def build(k, ra):
        rows, columns = block(k, ra)
        for h in range(HALVES):
            ids = slot_ids(back[k], h)
            w = jnp.zeros((KR, T), F32)
            for j in range(top):
                w += jnp.where(ids == meta[back[k], ra, j:j + 1, :], meta[back[k], ra, 8 + j:9 + j, :], 0.0)
            wg[rows, pl.ds(columns.start + h * KR, KR)] = w.T.astype(BF16)

    def partial(k, ra):
        rows = g_buf[k][:, :, :, ra].reshape(wide_w, parts[k])
        return jnp.dot(wg[block(k, ra)], rows, preferred_element_type=F32)

    relay_b2(1)
    for k in order:
        for h in range(HALVES):
            own_rows(k, h)
    for ra in [2, 1, 3, 0] if ring4 else range(R):
        for k in order:
            build(k, ra)
    for k in order:
        with jax.named_scope("wait_b2"):
            pend(whole(k, 0), b2_s.at[k, 0], b2_r.at[k, 0]).wait_recv()
    for k in order:
        with jax.named_scope("wait_b2"):
            pend(whole(k, 1), b2_s.at[k, 1], b2_r.at[k, 1]).wait_recv()

    def ps(k, ra, at):
        beside = k == 2 and parts[0] + parts[2] <= FF
        row = ((0 if beside else k) * (R - 1) + ra - 1) * T + at.start
        left = parts[0] if beside else 0
        return wu.at[pl.ds(row, at.size), pl.ds(left, parts[k])]

    def send_a2(k, ra, at):
        send(ps(k, ra, at), xa[k].at[R - ra, at], a2_s.at[k], a2_r.at[k], back[k], ra)

    if ring4:
        for k in order:
            with jax.named_scope("weigh_far"):
                ps(k, 2, pl.ds(0, T))[...] = partial(k, 2).astype(BF16)
            send(ps(k, 2, lo), xa[k].at[2, lo], a2_s.at[k], ah_r.at[k, 0], back[k], 1)
            send(ps(k, 2, hi), xa[k].at[2, hi], a2_s.at[k], ah_r.at[k, 1], back[k], 3)
        for k in order:
            with jax.named_scope("weigh_near"):
                for i, (ra, now, later) in enumerate(((1, hi, lo), (3, lo, hi))):
                    p = partial(k, ra)
                    ps(k, ra, now)[...] = p[now.start:now.start + now.size].astype(BF16)
                    send_a2(k, ra, now)
                    own[k][i] = p[later.start:later.start + later.size]
        for k in order:
            for i, (ra, at) in enumerate(((1, lo), (3, hi))):
                with jax.named_scope("weigh_sum"):
                    pend(xa[k].at[2, at], a2_s.at[k], ah_r.at[k, i]).wait_recv()
                    ps(k, ra, at)[...] = (own[k][i] + xa[k][2, at].astype(F32)).astype(BF16)
                    send_a2(k, ra, at)
    else:
        for k in order:
            for ra in range(1, R):
                ps(k, ra, pl.ds(0, T))[...] = partial(k, ra).astype(BF16)
                send_a2(k, ra, pl.ds(0, T))
    senders = (1, 3) if ring4 else tuple(range(1, R))

    for k in order:
        with jax.named_scope("weigh_own"):
            yacc[:, cols[k]] += partial(k, 0)
    for k in order:
        with jax.named_scope("wait_a2"):
            pend(xa[k].at[0:len(senders)], a2_s.at[k], a2_r.at[k]).wait_recv()
        total = yacc[:, cols[k]]
        for ra in senders:
            total += xa[k][ra].astype(F32)
        y_ref[:, cols[k]] = total.astype(BF16)
        pltpu.make_async_copy(y_ref.at[:, cols[k]], y_hbm.at[:, cols[k]], out_sem.at[k]).start()

    for k in range(3):
        pltpu.make_async_copy(y_ref.at[:, cols[k]], y_hbm.at[:, cols[k]], out_sem.at[k]).wait()
        pend(meta.at[k, 1:R], m_s.at[k], m_r.at[k]).wait_send()
        pend(xa[k].at[1:R], a2_s.at[k], a2_r.at[k]).wait_send()
        for h in range(HALVES):
            for s, r in ((c2_s, c2_r), (b2_s, b2_r)):
                pend(whole(k, h), s.at[k, h], r.at[k, h]).wait_send()


def hand_on(pieces, src, dst, held, in_sem, out_sem):
    n = src.shape[0] // pieces
    rows = [pl.ds(i * n, n) for i in range(pieces)]
    into = [pltpu.make_async_copy(src.at[r], held.at[r], in_sem.at[i]) for i, r in enumerate(rows)]
    out = [pltpu.make_async_copy(held.at[r], dst.at[r], out_sem.at[i]) for i, r in enumerate(rows)]
    for c in into:
        c.start()
    for a, b in zip(into, out):
        a.wait()
        b.start()
    for c in out:
        c.wait()


def split(d):
    tiles = d // 128
    low = tiles // 3
    sizes = [low, low, low]
    for i in range(tiles - 3 * low):
        sizes[2 - i] += 1
    return [128 * n for n in sizes]


def solution(mesh):
    names = ("dp", "ep")

    def step(x, expert, slot, gate, w_gate, w_up, w_down, s_gate, s_up, s_down):
        R = round(mesh.shape["ep"] ** (1 / 3))
        T, D = x.shape[2:]
        top, members = expert.shape[-1], mesh.shape["ep"]
        FF, SFF = w_gate.shape[-1], s_gate.shape[-1]
        slots = 5 * T * top // (4 * members)
        parts = split(D)
        x, (expert, slot, gate) = x[0, 0], (v[0].transpose(2, 0, 1) for v in (expert, slot, gate))
        any_space = pl.BlockSpec(memory_space=pl.ANY)
        tile = min(256, SFF)
        dma = pltpu.SemaphoreType.DMA
        scratch = (
            [pltpu.VMEM((R, T, c), BF16) for c in parts]
            + [pltpu.VMEM((HALVES, R, R, R, S, c), BF16) for c in parts]
            + [pltpu.VMEM((HALVES, R - 1, R, R, S, c), BF16) for c in parts]
            + [pltpu.VMEM((HALVES, R, R, R, S, c), BF16) for c in parts]
            + [pltpu.VMEM((2, T // 2, c), F32) for c in parts]
            + [pltpu.VMEM((T, D), BF16), pltpu.VMEM((T, D), BF16), pltpu.VMEM((top, 1, T), jnp.int32), pltpu.VMEM((top, 1, T), jnp.int32),
               pltpu.VMEM((top, 1, T), F32)]
            + [pltpu.VMEM((16, T), F32), pltpu.VMEM((3, R, 16, T), F32)]
            + [pltpu.VMEM((D, FF), BF16), pltpu.VMEM((D, FF), BF16), pltpu.VMEM((FF, D), BF16)]
            + [pltpu.VMEM((R * R * S, D), BF16), pltpu.VMEM((R * R * S, FF), BF16), pltpu.VMEM((T, D), F32)]
            + [pltpu.VMEM((2, D, tile), BF16), pltpu.VMEM((2, D, tile), BF16), pltpu.VMEM((2, tile, D), BF16)]
            + [dma((3,)), dma((4,)), dma((3,)), dma((2, 3))]
            + [dma((3,))] * 3 + [dma((3, R, 2))]
            + [dma((3, HALVES)), dma((3, HALVES, R)), dma((3, HALVES)), dma((3, HALVES))]
            + [dma((3, HALVES)), dma((3, HALVES, R)), dma((3, HALVES)), dma((3, HALVES))] + [dma((3,))] * 2 + [dma((3, 2))]
            + [pltpu.SemaphoreType.REGULAR((3, HALVES))] * 2
        )
        y = pl.pallas_call(
            functools.partial(kernel, R, parts, tile, top, slots, names),
            out_shape=jax.ShapeDtypeStruct((T, D), BF16),
            in_specs=[any_space] * 10,
            out_specs=any_space,
            scratch_shapes=scratch,
            compiler_params=pltpu.CompilerParams(
                collective_id=0, has_side_effects=True, vmem_limit_bytes=67043328
            ),
            name="moe",
        )(x, expert, slot, gate, w_gate[0], w_up[0], w_down[0], s_gate, s_up, s_down)
        pieces = 8
        y = pl.pallas_call(
            functools.partial(hand_on, pieces),
            out_shape=jax.ShapeDtypeStruct((T, D), BF16),
            in_specs=[any_space],
            out_specs=any_space,
            scratch_shapes=[pltpu.VMEM((T, D), BF16), dma((pieces,)), dma((pieces,))],
            name="hand_on",
        )(y)
        return y[None, None]

    tok = P("dp", "ep", None, None)
    exp = P("ep", None, None)
    rep = P(None, None)
    return jax.shard_map(
        step, mesh=mesh,
        in_specs=(tok, tok, tok, tok, exp, exp, exp, rep, rep, rep),
        out_specs=tok, check_vma=False,
    )
```
